256 devices in a mesh: gz: 32 (over z, x_hi, core), vert: 8 (over y, x_lo).
Axes of the slice: x: 4 (x_hi: 2, x_lo: 2; x = x_hi * 2 + x_lo), y: 4, z: 8, core: 2. Of those that a mesh axis runs over, the one named last changes fastest.
Arguments:
- volume: float32 [256, 128, 1024], P('gz'), may hold values from -6 to 6
- angle_index: int32 [32], P('vert'), may hold values from 0 to 511
- detector_rows: int32 [128], replicated, may hold values from 0 to 127, each once
- measured: float32 [32, 128, 1024], P('vert', 'gz'), may hold values from -96 to 96
Outputs:
- residual: float32 [32, 128, 1024], P('vert', 'gz')
- gradient: float32 [256, 128, 1024], P('gz', 'vert')
The draws below stay inside these ranges and needn't reach their ends.
All inputs are finite; a program needn't handle non-finite values.
Results may differ from the reference program's by a relative error of at most 0.0003.
Values sent between devices are 32-bit elements; how exact they have to be, the bound alone decides.
A program may use at most 64 MiB of HBM per device.

```python
import jax
import jax.numpy as jnp
from jax import lax

X = 1024
ANGLES = 512
NZ = 256
Y = 128
VIEWS = 32


def touch_ends(result, own_key, least, top_value):
    longest = result.shape.index(max(result.shape))
    spots = []
    for shift in (0, 1):
        where = [jax.random.randint(jax.random.fold_in(own_key, axis), (), 0, length) for axis, length in enumerate(result.shape)]
        where[longest] = (where[longest] + shift) % result.shape[longest]
        spots.append(tuple(where))
    return result.at[spots[0]].set(least).at[spots[1]].set(top_value)


def block_levels(rng, extent, pieces, least, high):
    loudness, own = 1.0, jax.random.fold_in(rng, 6)
    for axis_at, shards_of in pieces:
        heights = jnp.exp(jax.random.uniform(jax.random.fold_in(own, axis_at), (shards_of,), jnp.float32, least / len(pieces), high / len(pieces)))
        loudness = loudness * jnp.repeat(heights, extent[axis_at] // shards_of).reshape([-1 if axis == axis_at else 1 for axis in range(len(extent))])
    return loudness


def noise(key, dims, scale, reach, shards=(), kind=jnp.bfloat16):
    result = jax.random.normal(key, dims, jnp.float32) * scale
    if len(shards) > 0:
        result = block_levels(key, dims, shards, -0.22, 0.18) * result
    return jnp.clip(result, min=-reach, max=reach).astype(kind)


def setup_inputs(seed: int = 0) -> dict:
    streams_of = jax.random.split(jax.random.key(seed), 5)
    volume = noise(streams_of[0], (NZ, Y, X), 1.0, 6.0, ((0, 32),), jnp.float32)
    angle_index = touch_ends(jax.random.randint(streams_of[1], (VIEWS,), 0, ANGLES), jax.random.fold_in(streams_of[1], 1), 0, ANGLES - 1).astype(jnp.int32)
    detector_rows = jax.random.permutation(streams_of[2], Y).astype(jnp.int32)
    measured = noise(streams_of[3], (VIEWS, Y, X), 16.0, 96.0, ((0, 8), (1, 32)), jnp.float32)
    return {"volume": volume, "angle_index": angle_index, "detector_rows": detector_rows, "measured": measured}


def shifts(depth_pos, angle_value):
    slope_num = 2 * angle_value - ANGLES
    product = depth_pos * slope_num
    shift_whole = jnp.floor_divide(product, ANGLES)
    shift_part = (product - shift_whole * ANGLES).astype(jnp.float32) / ANGLES
    slope_value = slope_num.astype(jnp.float32) / ANGLES
    weight = jnp.sqrt(1.0 + slope_value * slope_value)
    return (shift_whole.astype(jnp.int32), shift_part, weight)

def reference(volume, angle_index, detector_rows, measured):
    margin = NZ // 2 + 2
    padded = jnp.pad(volume, ((0, 0), (0, 0), (margin, margin)))
    depth_pos = jnp.arange(NZ, dtype=jnp.int32) - NZ // 2

    def project(angle_value):
        shift_whole, shift_part, weight = shifts(depth_pos, angle_value)

        def shifted(plane, offset, fraction):
            window = lax.dynamic_slice_in_dim(plane, offset, X + 1, 1)
            return (1.0 - fraction) * window[:, :-1] + fraction * window[:, 1:]
        contrib = jax.vmap(shifted)(padded, margin + shift_whole, shift_part)
        return weight * lax.optimization_barrier(jnp.sum(contrib, axis=0))
    projection = lax.map(project, angle_index)
    det_order = jnp.take(projection, detector_rows, axis=1)
    residual = (det_order - measured) * NZ ** (-0.5)
    back = jnp.zeros_like(residual).at[:, detector_rows, :].set(residual)
    back_pad = jnp.pad(back, ((0, 0), (0, 0), (margin, margin)))

    def add_view(running, view_item):
        plane, angle_value = view_item
        shift_whole, shift_part, weight = shifts(depth_pos, angle_value)

        def shifted(offset, fraction):
            window = lax.dynamic_slice_in_dim(plane, offset, X + 1, 1)
            return (1.0 - fraction) * window[:, 1:] + fraction * window[:, :-1]
        contrib = jax.vmap(shifted)(margin - shift_whole - 1, shift_part)
        return (running + weight * contrib, None)
    start_sum = jnp.zeros((NZ, Y, X), jnp.float32)
    summed, _ = lax.scan(add_view, start_sum, (back_pad, angle_index))
    gradient = summed * VIEWS ** (-0.5)
    return (residual, gradient)
```

```python
import jax
import jax.numpy as jnp
from jax import lax
from jax.experimental import pallas as pl
from jax.experimental.pallas import tpu as pltpu
from jax.sharding import PartitionSpec as P

L = 128
CHIPS = 16
VERT = 8
VIEWS = 32
MID = 1
EXT = 56
F32 = jnp.float32
HIGH = lax.Precision.HIGHEST


def at(gz, vert):
    return {"gz": gz, "vert": vert}


def lane_iota(shape=(8, L)):
    return lax.broadcasted_iota(jnp.int32, shape, len(shape) - 1)


def sub_iota(shape=(8, L)):
    return lax.broadcasted_iota(jnp.int32, shape, len(shape) - 2)


def visit(i, p):
    step = lax.div(i, 2)
    far = lax.div(step + 1, 2)
    dz = jnp.where(lax.rem(step, 2) == 1, far, 8 - far)
    z = lax.rem(lax.div(p, 2) + dz, 8)
    return z * 2 + lax.rem(p + i, 2)


def row_of(ref, r):
    return jnp.broadcast_to(ref[pl.ds(r, 1), :], (8, L))


def extend(x, ext, base):
    lane = lane_iota()
    zero = jnp.zeros((8, L), F32)
    r1, r2, r3 = (pltpu.roll(x, L - n, 1) for n in (1, 2, 3))
    parts = (
        x,
        jnp.where(lane < 127, r1, zero),
        jnp.where(lane < 126, r2, zero),
        jnp.where(lane < 126, x, zero),
        jnp.where(lane == 126, zero, r1),
        r2,
        jnp.where(lane == 125, zero, r3),
    )
    for n, value in enumerate(parts):
        ext[base + 8 * n : base + 8 * n + 8, :] = value


def project_slab(chunk, slab, ext, phi_t, tab, part):
    lane = lane_iota()
    for zz in range(8):
        extend(chunk[zz], ext, zz * EXT)
    for v in range(VIEWS):
        acc = None
        for zz in range(8):
            off = tab[0, v, slab * 8 + zz] + zz * EXT
            a = ext[pl.ds(off, 8), :]
            b = ext[pl.ds(off + 1, 8), :]
            phi = row_of(phi_t.at[v], slab * 8 + zz)
            term = a + phi * (b - a)
            acc = term if acc is None else acc + term
        kc = tab[1, v, slab * 8]
        pos = lane + kc
        moved = pltpu.roll(acc, (L - kc) & (L - 1), 1)
        part[v] += jnp.where((pos >= -2) & (pos < L), moved, 0.0)


def backproject_slab(slab, bw, ext, phi_t, tab, out):
    lane = lane_iota()
    for v in range(VIEWS):
        kc = tab[3, v, slab * 8]
        row = bw[v]
        for n in range(3):
            pos = lane + (kc + n)
            moved = pltpu.roll(row, (2 * L - kc - n) & (L - 1), 1)
            ext[v * 24 + 8 * n : v * 24 + 8 * n + 8, :] = jnp.where((pos >= 0) & (pos < L), moved, 0.0)
    for zz in range(8):
        acc = None
        for v in range(VIEWS):
            off = tab[2, v, slab * 8 + zz] + v * 24
            b = ext[pl.ds(off, 8), :]
            a = ext[pl.ds(off + 1, 8), :]
            phi = row_of(phi_t.at[v], slab * 8 + zz)
            term = a + phi * (b - a)
            acc = term if acc is None else acc + term
        out[zz] = acc


def to_tiles(read, batch, turned, tiles):
    for t in range(8):
        turned[t * L : (t + 1) * L, 0:batch] = jnp.transpose(read(t))
    for r in range(8):
        tiles[r * batch : (r + 1) * batch, :] = jnp.transpose(turned[pl.ds(r, L, stride=8), 0:batch])


def one_hot(dr, bit):
    lane = lane_iota((8, L))
    wide = jnp.broadcast_to(dr, (8, L))
    halves = []
    for half in range(2):
        src = half * 64 + (lane // 8) * 4 + lane % 4
        got = jnp.take_along_axis(wide, src, axis=1, mode="promise_in_bounds")
        got = jnp.where((lane // 4) % 2 == bit, got, -1)
        halves.append(jnp.broadcast_to(got[0:1], (L, L)))
    row = lax.broadcasted_iota(jnp.int32, (L, 2 * L), 0)
    return (jnp.concatenate(halves, axis=1) == row).astype(F32)


def kernel(
    volume, angles, det, measured,
    grad_in, res_in,
    vb, mbuf, m16, turned, tiles, xsend, xin, abuf, sf, wt, tab_v, phi_t, ext, ext_b,
    part, pin, bw, mtiles, mi, mr, m2, msend, m3, rsend, r2, rs2, r3, xres, gsend, tab,
    loc_sem, vol_send, vol_recv, ang_send, ang_recv, part_send, part_recv,
    mid_send, mid_recv, grad_send, grad_recv,
):
    gz, vert = lax.axis_index("gz"), lax.axis_index("vert")
    p, core = lax.div(gz, 2), lax.rem(gz, 2)
    barrier = pltpu.get_barrier_semaphore()

    load_v = pltpu.make_async_copy(volume.at[:, pl.ds(pl.multiple_of(vert * 16, 16), 16), :], vb, loc_sem.at[0])
    load_m = pltpu.make_async_copy(measured, mbuf, loc_sem.at[1])
    load_v.start()
    load_m.start()

    def greet_gz(i, _):
        pl.semaphore_signal(barrier, inc=1, device_id=at(lax.rem(gz + i, 32), vert))
        return 0

    def greet_vert(i, _):
        pl.semaphore_signal(barrier, inc=1, device_id=at(gz, lax.rem(vert + i, VERT)))
        return 0

    lax.fori_loop(1, 32, greet_gz, 0)
    lax.fori_loop(1, VERT, greet_vert, 0)

    sub = sub_iota()
    slope = jnp.zeros((8, L), jnp.int32)
    for i in range(4):
        slope = jnp.where(sub % 4 == i, jnp.full((8, L), 2 * angles[i] - 512), slope)
    abuf[vert] = slope
    part[...] = jnp.zeros_like(part)

    load_m.wait()
    for a in range(4):
        m16[4 * a : 4 * a + 4, :] = mbuf[a]
    to_tiles(lambda t: m16[:, t * L : (t + 1) * L], 16, turned, mtiles)
    load_v.wait()
    to_tiles(lambda t: vb[:, :, t * L : (t + 1) * L].reshape(L, L), L, turned, tiles)

    def gather_rows(q, _):
        for zz in range(8):
            xsend[q, zz] = tiles[pl.ds(zz * 16 + q, 8, stride=L), :]
        return 0

    lax.fori_loop(0, CHIPS, gather_rows, 0)
    for zz in range(8):
        xin[p, zz] = xsend[p, zz]

    pl.semaphore_wait(barrier, 31 + 7)

    def send_angles(i, _):
        pltpu.make_async_remote_copy(
            abuf.at[vert], abuf.at[vert], ang_send, ang_recv, device_id=at(gz, lax.rem(vert + i, VERT))
        ).start()
        return 0

    lax.fori_loop(1, VERT, send_angles, 0)

    def measured_chunk(q):
        return mtiles.at[pl.ds(pl.multiple_of(lax.rem(q, 8) * 16 + lax.div(q, 8) * 8, 8), 8)]

    def send_measured(i, _):
        q = lax.rem(p + i, CHIPS)

        @pl.when(q * 2 + MID != gz)
        def _():
            pltpu.make_async_remote_copy(
                measured_chunk(q), mi.at[gz], mid_send.at[0], mid_recv.at[0], device_id=at(q * 2 + MID, vert)
            ).start()

        return 0

    lax.fori_loop(0, CHIPS, send_measured, 0)

    def vol_copy(i):
        q = visit(i, p)
        return pltpu.make_async_remote_copy(
            xsend.at[q], xin.at[p], vol_send, vol_recv.at[p], device_id=at(q * 2 + core, vert)
        )

    def send_volume(i, _):
        vol_copy(i).start()
        return 0

    lax.fori_loop(1, CHIPS, send_volume, 0)

    @pl.when(core == MID)
    def _():
        mi[gz] = measured_chunk(p)[...]

    pltpu.make_async_copy(abuf.at[pl.ds(0, 7)], abuf.at[pl.ds(0, 7)], ang_recv).wait()
    for g in range(4):
        tab_v[0, 8 * g : 8 * g + 8, :] = jnp.where(sub < 4, abuf[2 * g], abuf[2 * g + 1])
    s = tab_v[0]
    sf[...] = s.astype(F32)
    slope_value = sf[...] * (1.0 / 512)
    wt[...] = jnp.sqrt(1.0 + slope_value * slope_value)
    lane = lane_iota((VIEWS, L))
    first = 16 * (lane // 8) + 8 * core - 128
    ends = ((first * s) >> 9, ((first + 7) * s) >> 9)
    k_min, k_max = jnp.minimum(*ends), jnp.maximum(*ends)
    k = ((first + lane % 8) * s) >> 9
    kc = jnp.where(k_min < 0, jnp.minimum(k_min >> 3, -2), k_min >> 3)
    tab_v[0] = k - 8 * kc + jnp.where(k_min < 0, 24, 0)
    tab_v[1] = kc
    kb = (-k_max - 1) >> 3
    tab_v[2] = -k - 1 - 8 * kb
    tab_v[3] = kb
    to_smem = pltpu.make_async_copy(tab_v, tab, loc_sem.at[2])
    to_smem.start()

    def fill_phi(v, _):
        sv = row_of(sf, v)
        for slab in range(CHIPS):
            q = (16 * slab + 8 * core - 128 + sub).astype(F32) * sv * (1.0 / 512)
            phi_t[v, slab * 8 : slab * 8 + 8, :] = q - jnp.floor(q)
        return 0

    lax.fori_loop(0, VIEWS, fill_phi, 0)
    to_smem.wait()

    def project_step(i, _):
        q = visit(i, p)

        @pl.when(i > 0)
        def _():
            pltpu.make_async_copy(xin.at[q], xin.at[q], vol_recv.at[q]).wait()

        project_slab(xin.at[q], q, ext, phi_t, tab, part)

        @pl.when((core == MID) & (i == 3))
        def _():
            pltpu.make_async_copy(mi.at[pl.ds(0, 31)], mi.at[pl.ds(0, 31)], mid_recv.at[0]).wait()
            got = mi[...].reshape(2 * L, L)
            for bit in range(2):
                rows = jnp.dot(one_hot(det[...], bit), got, precision=HIGH, preferred_element_type=F32)
                mr[:, bit] = rows.reshape(VERT, 16, L)

            def send(n, _):
                w = lax.rem(vert + n, VERT)
                pltpu.make_async_remote_copy(
                    mr.at[w], m2.at[vert], mid_send.at[1], mid_recv.at[1], device_id=at(gz, w)
                ).start()
                return 0

            lax.fori_loop(1, VERT, send, 0)
            m2[vert] = mr[vert]

        @pl.when((core == MID) & (i == 7))
        def _():
            pltpu.make_async_copy(m2.at[pl.ds(0, 7)], m2.at[pl.ds(0, 7)], mid_recv.at[1]).wait()
            flat = m2.reshape(256, L)
            for q in range(CHIPS):
                msend[q] = flat[pl.ds(q, 16, stride=16), :]

            def send(n, _):
                w = lax.rem(p + n, CHIPS)
                pltpu.make_async_remote_copy(
                    msend.at[w], m3.at[p], mid_send.at[2], mid_recv.at[2], device_id=at(w * 2 + MID, vert)
                ).start()
                return 0

            lax.fori_loop(1, CHIPS, send, 0)
            m3[p] = msend[p]

        return 0

    lax.fori_loop(0, CHIPS, project_step, 0)

    for v in range(VIEWS):
        part[v] = part[v] * row_of(wt, v)

    @pl.when(core == MID)
    def _():
        pltpu.make_async_copy(m3.at[pl.ds(0, 15)], m3.at[pl.ds(0, 15)], mid_recv.at[2]).wait()
        flat = m3.reshape(256, L)
        for v in range(VIEWS):
            w, pair, bit = v // 4, (v % 4) // 2, v % 2
            part[v] = part[v] - flat[pl.ds(pair * 128 + 2 * w + bit, 8, stride=16), :]

    swap = pltpu.make_async_remote_copy(part, pin, part_send, part_recv, device_id=at(gz + 1 - 2 * core, vert))
    swap.start()
    swap.wait()
    for v in range(VIEWS):
        value = (part[v] + pin[v]) * (1.0 / 16)
        pin[v] = value
        bw[v] = value * row_of(wt, v) * (VIEWS**-0.5)

    flat_res = pin.reshape(VIEWS * 8, L)
    for b in range(8):
        for bit in range(2):
            rsend[b, 8 * bit : 8 * bit + 8, :] = flat_res[pl.ds((2 * core + bit) * 8 + b, 8, stride=32), :]

    def send_residual(b, _):
        q = core * 8 + b

        @pl.when(q * 2 + MID != gz)
        def _():
            pltpu.make_async_remote_copy(
                rsend.at[b], r2.at[p], mid_send.at[3], mid_recv.at[3], device_id=at(q * 2 + MID, vert)
            ).start()

        return 0

    lax.fori_loop(0, 8, send_residual, 0)
    own_mid = (core == MID) & (lax.div(p, 8) == MID)

    @pl.when(own_mid)
    def _():
        r2[p] = rsend[lax.rem(p, 8)]

    def grad_copy(q):
        return pltpu.make_async_remote_copy(
            gsend.at[q], grad_in.at[p], grad_send, grad_recv, device_id=at(q * 2 + core, vert)
        )

    def back_step(i, _):
        q = visit(CHIPS - 1 - i, p)
        backproject_slab(q, bw, ext_b, phi_t, tab, gsend.at[q])

        @pl.when(i < CHIPS - 1)
        def _():
            grad_copy(q).start()

        @pl.when((core == MID) & (i == 3))
        def _():
            @pl.when(own_mid)
            def _():
                pltpu.make_async_copy(r2.at[pl.ds(0, 15)], r2.at[pl.ds(0, 15)], mid_recv.at[3]).wait()

            @pl.when(jnp.logical_not(own_mid))
            def _():
                pltpu.make_async_copy(r2, r2, mid_recv.at[3]).wait()

            flat = r2.reshape(256, L)
            for w in range(VERT):
                for bit in range(2):
                    rs2[w, bit] = flat[pl.ds(bit * 8 + w, 16, stride=16), :]

            def send(n, _):
                w = lax.rem(vert + n, VERT)
                pltpu.make_async_remote_copy(
                    rs2.at[w], r3.at[vert], mid_send.at[4], mid_recv.at[4], device_id=at(gz, w)
                ).start()
                return 0

            lax.fori_loop(1, VERT, send, 0)
            r3[vert] = rs2[vert]

        @pl.when((core == MID) & (i == 7))
        def _():
            pltpu.make_async_copy(r3.at[pl.ds(0, 7)], r3.at[pl.ds(0, 7)], mid_recv.at[4]).wait()
            total = None
            for bit in range(2):
                rows = r3[:, bit].reshape(L, L)
                hot = jnp.transpose(one_hot(det[...], bit))
                out = jnp.dot(hot, rows, precision=HIGH, preferred_element_type=F32)
                total = out if total is None else total + out
            xres[...] = total.reshape(32, 8, L)

            def send(n, _):
                w = lax.rem(gz + n, 32)
                pltpu.make_async_remote_copy(
                    xres.at[w], res_in.at[p], mid_send.at[5], mid_recv.at[5], device_id=at(w, vert)
                ).start()
                return 0

            lax.fori_loop(1, 32, send, 0)
            pltpu.make_async_copy(xres.at[gz], res_in.at[p], loc_sem.at[3]).start()

        return 0

    lax.fori_loop(0, CHIPS, back_step, 0)
    own_grad = pltpu.make_async_copy(gsend.at[p], grad_in.at[p], loc_sem.at[4])
    own_grad.start()

    pltpu.make_async_copy(abuf.at[pl.ds(0, 7)], abuf.at[pl.ds(0, 7)], ang_send).wait()
    pltpu.make_async_copy(xin.at[pl.ds(0, 15)], xin.at[pl.ds(0, 15)], vol_send).wait()

    @pl.when(core == MID)
    def _():
        pltpu.make_async_copy(mi.at[pl.ds(0, 15)], mi.at[pl.ds(0, 15)], mid_send.at[0]).wait()
        pltpu.make_async_copy(m2.at[pl.ds(0, 7)], m2.at[pl.ds(0, 7)], mid_send.at[1]).wait()
        pltpu.make_async_copy(m3.at[pl.ds(0, 15)], m3.at[pl.ds(0, 15)], mid_send.at[2]).wait()
        pltpu.make_async_copy(r3.at[pl.ds(0, 7)], r3.at[pl.ds(0, 7)], mid_send.at[4]).wait()
        pltpu.make_async_copy(xres.at[pl.ds(0, 31)], xres.at[pl.ds(0, 31)], mid_send.at[5]).wait()
        pltpu.make_async_copy(xres.at[gz], res_in.at[p], loc_sem.at[3]).wait()
        pltpu.make_async_copy(res_in.at[pl.ds(0, 15)], res_in.at[pl.ds(0, 15)], mid_recv.at[5]).wait()

    @pl.when(core != MID)
    def _():
        pltpu.make_async_copy(mi.at[pl.ds(0, 16)], mi.at[pl.ds(0, 16)], mid_send.at[0]).wait()
        pltpu.make_async_copy(res_in, res_in, mid_recv.at[5]).wait()

    @pl.when(own_mid)
    def _():
        pltpu.make_async_copy(rsend.at[pl.ds(0, 7)], rsend.at[pl.ds(0, 7)], mid_send.at[3]).wait()

    @pl.when(jnp.logical_not(own_mid))
    def _():
        pltpu.make_async_copy(rsend, rsend, mid_send.at[3]).wait()

    own_grad.wait()
    pltpu.make_async_copy(gsend.at[pl.ds(0, 15)], gsend.at[pl.ds(0, 15)], grad_send).wait()
    pltpu.make_async_copy(grad_in.at[pl.ds(0, 15)], grad_in.at[pl.ds(0, 15)], grad_recv).wait()


def exchange(volume, angles, det, measured):
    dma = pltpu.SemaphoreType.DMA
    any_space = pl.BlockSpec(memory_space=pl.ANY)
    vmem = lambda *dims, dtype=F32: pltpu.VMEM(dims, dtype)
    scratch = [
        vmem(8, 16, 1024), vmem(4, 4, 1024), vmem(16, 1024), vmem(1024, L), vmem(1024, L),
        vmem(CHIPS, 8, 8, L), vmem(CHIPS, 8, 8, L), vmem(VERT, 8, L, dtype=jnp.int32), vmem(VIEWS, L), vmem(VIEWS, L),
        vmem(4, VIEWS, L, dtype=jnp.int32), vmem(VIEWS, L, L), vmem(8 * EXT, L), vmem(VIEWS * 24, L),
        vmem(VIEWS, 8, L), vmem(VIEWS, 8, L), vmem(VIEWS, 8, L), vmem(L, L), vmem(32, 8, L), vmem(VERT, 2, 16, L),
        vmem(VERT, 2, 16, L), vmem(CHIPS, 16, L), vmem(CHIPS, 16, L), vmem(8, 16, L), vmem(CHIPS, 16, L),
        vmem(VERT, 2, 16, L), vmem(VERT, 2, 16, L), vmem(32, 8, L), vmem(CHIPS, 8, 8, L),
        pltpu.SMEM((4, VIEWS, L), jnp.int32),
        dma((5,)), dma, dma((CHIPS,)), dma, dma, dma, dma, dma((6,)), dma((6,)), dma, dma,
    ]
    return pl.pallas_call(
        kernel,
        out_shape=[jax.ShapeDtypeStruct((CHIPS, 8, 8, L), F32), jax.ShapeDtypeStruct((CHIPS, 8, L), F32)],
        in_specs=[
            any_space,
            pl.BlockSpec(memory_space=pltpu.SMEM),
            pl.BlockSpec(memory_space=pltpu.VMEM),
            any_space,
        ],
        out_specs=[any_space, any_space],
        scratch_shapes=scratch,
        compiler_params=pltpu.CompilerParams(collective_id=0, has_side_effects=True, vmem_limit_bytes=40 * 2**20),
        name="exchange",
    )(volume, angles, det, measured)


def finish_kernel(grad_in, res_in, res_out, grad_out, turned):
    for r in range(8):
        both = jnp.concatenate([res_in[r], res_in[8 + r]], axis=0)
        turned[pl.ds(r, L, stride=8), 0:16] = jnp.transpose(both)
    for t in range(8):
        rows = jnp.transpose(turned[t * L : (t + 1) * L, 0:16])
        for a in range(4):
            res_out[a, :, t * L : (t + 1) * L] = rows[4 * a : 4 * a + 4]
    flat = grad_in.reshape(CHIPS * 64, L)
    for r in range(8):
        rows = [flat[pl.ds(zz * 8 + r, 16, stride=64), :] for zz in range(8)]
        turned[pl.ds(r, L, stride=8), :] = jnp.transpose(jnp.concatenate(rows, axis=0))
    for t in range(8):
        grad_out[:, :, t * L : (t + 1) * L] = jnp.transpose(turned[t * L : (t + 1) * L, :]).reshape(8, 16, L)


def finish(grad_in, res_in):
    return pl.pallas_call(
        finish_kernel,
        out_shape=[jax.ShapeDtypeStruct((4, 4, 1024), F32), jax.ShapeDtypeStruct((8, 16, 1024), F32)],
        in_specs=[pl.BlockSpec(memory_space=pltpu.VMEM)] * 2,
        out_specs=[pl.BlockSpec(memory_space=pltpu.VMEM)] * 2,
        scratch_shapes=[pltpu.VMEM((1024, L), F32)],
        name="finish",
    )(grad_in, res_in)


def per_device(volume, angle_index, detector_rows, measured):
    grad_in, res_in = exchange(volume, angle_index, detector_rows.reshape(1, L), measured)
    residual, gradient = finish(grad_in, res_in)
    return residual, gradient


def solution(mesh):
    in_specs = (P("gz", None, None), P("vert"), P(), P("vert", "gz", None))
    out_specs = (P("vert", "gz", None), P("gz", "vert", None))
    return jax.shard_map(per_device, mesh=mesh, in_specs=in_specs, out_specs=out_specs, check_vma=False)
```

```python
import jax
import jax.numpy as jnp
from jax import lax
from jax.experimental import pallas as pl
from jax.experimental.pallas import tpu as pltpu
from jax.sharding import PartitionSpec as P

L = 128
CHIPS = 16
VERT = 8
VIEWS = 32
GROUP = 8
AT_ONCE = 2
FORWARD_AT = 6
BACK_AT = 9
MID = 1
EXT = 56
F32 = jnp.float32
ALL_VMEM = 62 * 2**20
HIGH = lax.Precision.HIGHEST


def at(gz, vert):
    return {"gz": gz, "vert": vert}


def lane_iota(shape=(8, L)):
    return lax.broadcasted_iota(jnp.int32, shape, len(shape) - 1)


def sub_iota(shape=(8, L)):
    return lax.broadcasted_iota(jnp.int32, shape, len(shape) - 2)


def visit(i, p):
    step = lax.div(i, 2)
    far = lax.div(step + 1, 2)
    dz = jnp.where(lax.rem(step, 2) == 1, far, 8 - far)
    z = lax.rem(lax.div(p, 2) + dz, 8)
    return z * 2 + lax.rem(p + i, 2)


def row_of(ref, r):
    return jnp.broadcast_to(ref[pl.ds(r, 1), :], (8, L))


def extend(x, ext, base):
    lane = lane_iota()
    zero = jnp.zeros((8, L), F32)
    r1, r2, r3 = (pltpu.roll(x, L - n, 1) for n in (1, 2, 3))
    parts = (
        x,
        jnp.where(lane < 127, r1, zero),
        jnp.where(lane < 126, r2, zero),
        jnp.where(lane < 126, x, zero),
        jnp.where(lane == 126, zero, r1),
        r2,
        jnp.where(lane == 125, zero, r3),
    )
    for n, value in enumerate(parts):
        ext[base + 8 * n : base + 8 * n + 8, :] = value


def project_slab(chunk, slab, ext, phi_t, tab, part, accs):
    lane = lane_iota()
    for zz in range(8):
        extend(chunk[zz], ext, zz * EXT)

    def some_views(g, _):
        offs = tab.at[0, pl.ds(g * GROUP, GROUP), pl.ds(slab * 8, 8)]
        phis = phi_t.at[pl.ds(g * GROUP, GROUP), pl.ds(slab * 8, 8), :]
        for j in range(GROUP):
            acc = None
            for zz in range(8):
                off = offs[j, zz]
                a = ext[pl.ds(off, 8), :]
                b = ext[pl.ds(off + 1, 8), :]
                term = a + row_of(phis.at[j], zz) * (b - a)
                acc = term if acc is None else acc + term
            accs[g * GROUP + j] = acc
        return 0

    lax.fori_loop(0, VIEWS // GROUP, some_views, 0)
    kcs = tab.at[1, :, pl.ds(slab * 8, 8)]
    for v in range(VIEWS):
        kc = kcs[v, 0]
        pos = lane + kc
        moved = pltpu.roll(accs[v], (L - kc) & (L - 1), 1)
        part[v] += jnp.where((pos >= -2) & (pos < L), moved, 0.0)


def backproject_slab(slab, bw, ext, phi_t, tab, out):
    lane = lane_iota()
    kcs = tab.at[3, :, pl.ds(slab * 8, 8)]
    for v in range(VIEWS):
        kc = kcs[v, 0]
        row = bw[v]
        for n in range(3):
            pos = lane + (kc + n)
            moved = pltpu.roll(row, (2 * L - kc - n) & (L - 1), 1)
            ext[v * 24 + 8 * n : v * 24 + 8 * n + 8, :] = jnp.where((pos >= 0) & (pos < L), moved, 0.0)

    def layers(n, _):
        offs = tab.at[2, :, pl.ds(slab * 8 + n * AT_ONCE, AT_ONCE)]
        phis = phi_t.at[:, pl.ds(slab * 8 + n * AT_ONCE, AT_ONCE), :]
        for zz in range(AT_ONCE):
            accs = [None] * 4
            for v in range(VIEWS):
                off = offs[v, zz]
                b = ext[pl.ds(off, 8), :]
                a = ext[pl.ds(off + 1, 8), :]
                term = a + row_of(phis.at[v], zz) * (b - a)
                accs[v % 4] = term if v < 4 else accs[v % 4] + term
            out[n * AT_ONCE + zz] = (accs[0] + accs[1]) + (accs[2] + accs[3])
        return 0

    lax.fori_loop(0, 8 // AT_ONCE, layers, 0)


def to_tiles(read, batch, turned, tiles):
    for t in range(8):
        turned[t * L : (t + 1) * L, 0:batch] = jnp.transpose(read(t))
    for r in range(8):
        tiles[r * batch : (r + 1) * batch, :] = jnp.transpose(turned[pl.ds(r, L, stride=8), 0:batch])


def one_hot(dr, bit):
    lane = lane_iota((8, L))
    wide = jnp.broadcast_to(dr, (8, L))
    halves = []
    for half in range(2):
        src = half * 64 + (lane // 8) * 4 + lane % 4
        got = jnp.take_along_axis(wide, src, axis=1, mode="promise_in_bounds")
        got = jnp.where((lane // 4) % 2 == bit, got, -1)
        halves.append(jnp.broadcast_to(got[0:1], (L, L)))
    row = lax.broadcasted_iota(jnp.int32, (L, 2 * L), 0)
    return (jnp.concatenate(halves, axis=1) == row).astype(F32)


def kernel(
    volume, angles_in, det_in, measured,
    grad_in, res_in,
    vb, mbuf, m16, turned, tiles, xsend, xin, abuf, sf, wt, tab_v, phi_t, ext, ext_b,
    part, pin, bw, mtiles, mi, mr, m2, msend, m3, rsend, r2, rs2, r3, xres, gsend, accs, hot, hot_t, det, tab, angles,
    loc_sem, vol_send, vol_recv, ang_send, ang_recv, part_send, part_recv,
    mid_send, mid_recv, grad_send, grad_recv,
):
    gz, vert = lax.axis_index("gz"), lax.axis_index("vert")
    p, core = lax.div(gz, 2), lax.rem(gz, 2)
    barrier = pltpu.get_barrier_semaphore()

    load_v = pltpu.make_async_copy(volume.at[:, pl.ds(pl.multiple_of(vert * 16, 16), 16), :], vb, loc_sem.at[0])
    load_m = pltpu.make_async_copy(measured, mbuf, loc_sem.at[1])
    load_a = pltpu.make_async_copy(angles_in, angles, loc_sem.at[3])
    load_d = pltpu.make_async_copy(det_in, det, loc_sem.at[4])
    for load in (load_a, load_v, load_m, load_d):
        load.start()

    def greet_gz(i, _):
        pl.semaphore_signal(barrier, inc=1, device_id=at(lax.rem(gz + i, 32), vert))
        return 0

    def greet_vert(i, _):
        pl.semaphore_signal(barrier, inc=1, device_id=at(gz, lax.rem(vert + i, VERT)))
        return 0

    lax.fori_loop(1, 32, greet_gz, 0)
    lax.fori_loop(1, VERT, greet_vert, 0)

    sub = sub_iota()
    load_a.wait()
    load_d.wait()
    slope = jnp.zeros((8, L), jnp.int32)
    for i in range(4):
        slope = jnp.where(sub % 4 == i, jnp.full((8, L), 2 * angles[i] - 512), slope)
    abuf[vert] = slope
    part[...] = jnp.zeros_like(part)

    load_m.wait()
    for a in range(4):
        m16[4 * a : 4 * a + 4, :] = mbuf[a]
    to_tiles(lambda t: m16[:, t * L : (t + 1) * L], 16, turned, mtiles)
    load_v.wait()
    to_tiles(lambda t: vb[:, :, t * L : (t + 1) * L].reshape(L, L), L, turned, tiles)

    def gather_rows(q, _):
        for zz in range(8):
            xsend[q, zz] = tiles[pl.ds(zz * 16 + q, 8, stride=L), :]
        return 0

    lax.fori_loop(0, CHIPS, gather_rows, 0)
    for zz in range(8):
        xin[p, zz] = xsend[p, zz]

    @pl.when(core == MID)
    def _():
        for bit in range(2):
            hot[bit] = one_hot(det[...], bit)
            hot_t[bit] = jnp.transpose(hot[bit])

    pl.semaphore_wait(barrier, 31 + 7)

    def send_angles(i, _):
        pltpu.make_async_remote_copy(
            abuf.at[vert], abuf.at[vert], ang_send, ang_recv, device_id=at(gz, lax.rem(vert + i, VERT))
        ).start()
        return 0

    lax.fori_loop(1, VERT, send_angles, 0)

    def measured_chunk(q):
        return mtiles.at[pl.ds(pl.multiple_of(lax.rem(q, 8) * 16 + lax.div(q, 8) * 8, 8), 8)]

    def send_measured(i, _):
        q = lax.rem(p + i, CHIPS)

        @pl.when(q * 2 + MID != gz)
        def _():
            pltpu.make_async_remote_copy(
                measured_chunk(q), mi.at[gz], mid_send.at[0], mid_recv.at[0], device_id=at(q * 2 + MID, vert)
            ).start()

        return 0

    lax.fori_loop(0, CHIPS, send_measured, 0)

    def vol_copy(i):
        q = visit(i, p)
        return pltpu.make_async_remote_copy(
            xsend.at[q], xin.at[p], vol_send, vol_recv.at[p], device_id=at(q * 2 + core, vert)
        )

    def send_volume(i, _):
        vol_copy(i).start()
        return 0

    lax.fori_loop(1, CHIPS, send_volume, 0)

    @pl.when(core == MID)
    def _():
        mi[gz] = measured_chunk(p)[...]

    pltpu.make_async_copy(abuf.at[pl.ds(0, 7)], abuf.at[pl.ds(0, 7)], ang_recv).wait()
    for g in range(4):
        tab_v[0, 8 * g : 8 * g + 8, :] = jnp.where(sub < 4, abuf[2 * g], abuf[2 * g + 1])
    s = tab_v[0]
    sf[...] = s.astype(F32)
    slope_value = sf[...] * (1.0 / 512)
    wt[...] = jnp.sqrt(1.0 + slope_value * slope_value)
    lane = lane_iota((VIEWS, L))
    first = 16 * (lane // 8) + 8 * core - 128
    ends = ((first * s) >> 9, ((first + 7) * s) >> 9)
    k_min, k_max = jnp.minimum(*ends), jnp.maximum(*ends)
    k = ((first + lane % 8) * s) >> 9
    kc = jnp.where(k_min < 0, jnp.minimum(k_min >> 3, -2), k_min >> 3)
    tab_v[0] = k - 8 * kc + jnp.where(k_min < 0, 24, 0) + (lane % 8) * EXT
    tab_v[1] = kc
    kb = (-k_max - 1) >> 3
    tab_v[2] = -k - 1 - 8 * kb + 24 * lax.broadcasted_iota(jnp.int32, (VIEWS, L), 0)
    tab_v[3] = kb
    to_smem = pltpu.make_async_copy(tab_v, tab, loc_sem.at[2])
    to_smem.start()

    def fill_phi(v, _):
        sv = row_of(sf, v)
        for slab in range(CHIPS):
            q = (16 * slab + 8 * core - 128 + sub).astype(F32) * sv * (1.0 / 512)
            phi_t[v, slab * 8 : slab * 8 + 8, :] = q - jnp.floor(q)
        return 0

    lax.fori_loop(0, VIEWS, fill_phi, 0)

    @pl.when(core == MID)
    def _():
        pltpu.make_async_copy(mi.at[pl.ds(0, 31)], mi.at[pl.ds(0, 31)], mid_recv.at[0]).wait()
        got = mi[...].reshape(2 * L, L)
        for bit in range(2):
            rows = jnp.dot(hot[bit], got, precision=HIGH, preferred_element_type=F32)
            mr[:, bit] = rows.reshape(VERT, 16, L)

        def send(n, _):
            w = lax.rem(vert + n, VERT)
            pltpu.make_async_remote_copy(
                mr.at[w], m2.at[vert], mid_send.at[1], mid_recv.at[1], device_id=at(gz, w)
            ).start()
            return 0

        lax.fori_loop(1, VERT, send, 0)
        m2[vert] = mr[vert]

    to_smem.wait()

    def project_step(i, _):
        q = visit(i, p)

        @pl.when(i > 0)
        def _():
            pltpu.make_async_copy(xin.at[q], xin.at[q], vol_recv.at[q]).wait()

        project_slab(xin.at[q], q, ext, phi_t, tab, part, accs)

        @pl.when((core == MID) & (i == FORWARD_AT))
        def _():
            pltpu.make_async_copy(m2.at[pl.ds(0, 7)], m2.at[pl.ds(0, 7)], mid_recv.at[1]).wait()
            flat = m2.reshape(256, L)
            for q in range(CHIPS):
                msend[q] = flat[pl.ds(q, 16, stride=16), :]

            def send(n, _):
                w = lax.rem(p + n, CHIPS)
                pltpu.make_async_remote_copy(
                    msend.at[w], m3.at[p], mid_send.at[2], mid_recv.at[2], device_id=at(w * 2 + MID, vert)
                ).start()
                return 0

            lax.fori_loop(1, CHIPS, send, 0)
            m3[p] = msend[p]

        return 0

    lax.fori_loop(0, CHIPS, project_step, 0)

    for v in range(VIEWS):
        part[v] = part[v] * row_of(wt, v)

    @pl.when(core == MID)
    def _():
        pltpu.make_async_copy(m3.at[pl.ds(0, 15)], m3.at[pl.ds(0, 15)], mid_recv.at[2]).wait()
        flat = m3.reshape(256, L)
        for v in range(VIEWS):
            w, pair, bit = v // 4, (v % 4) // 2, v % 2
            part[v] = part[v] - flat[pl.ds(pair * 128 + 2 * w + bit, 8, stride=16), :]

    swap = pltpu.make_async_remote_copy(part, pin, part_send, part_recv, device_id=at(gz + 1 - 2 * core, vert))
    swap.start()
    swap.wait()
    for v in range(VIEWS):
        value = (part[v] + pin[v]) * (1.0 / 16)
        pin[v] = value
        bw[v] = value * row_of(wt, v) * (VIEWS**-0.5)

    flat_res = pin.reshape(VIEWS * 8, L)
    for b in range(8):
        for bit in range(2):
            rsend[b, 8 * bit : 8 * bit + 8, :] = flat_res[pl.ds((2 * core + bit) * 8 + b, 8, stride=32), :]

    def send_residual(b, _):
        q = core * 8 + b

        @pl.when(q * 2 + MID != gz)
        def _():
            pltpu.make_async_remote_copy(
                rsend.at[b], r2.at[p], mid_send.at[3], mid_recv.at[3], device_id=at(q * 2 + MID, vert)
            ).start()

        return 0

    lax.fori_loop(0, 8, send_residual, 0)
    own_mid = (core == MID) & (lax.div(p, 8) == MID)

    @pl.when(own_mid)
    def _():
        r2[p] = rsend[lax.rem(p, 8)]

    def grad_copy(q):
        return pltpu.make_async_remote_copy(
            gsend.at[q], grad_in.at[p], grad_send, grad_recv, device_id=at(q * 2 + core, vert)
        )

    def back_step(i, _):
        q = visit(CHIPS - 1 - i, p)
        backproject_slab(q, bw, ext_b, phi_t, tab, gsend.at[q])

        @pl.when(i < CHIPS - 1)
        def _():
            grad_copy(q).start()

        @pl.when((core == MID) & (i == BACK_AT))
        def _():
            @pl.when(own_mid)
            def _():
                pltpu.make_async_copy(r2.at[pl.ds(0, 15)], r2.at[pl.ds(0, 15)], mid_recv.at[3]).wait()

            @pl.when(jnp.logical_not(own_mid))
            def _():
                pltpu.make_async_copy(r2, r2, mid_recv.at[3]).wait()

            flat = r2.reshape(256, L)
            for w in range(VERT):
                for bit in range(2):
                    rs2[w, bit] = flat[pl.ds(bit * 8 + w, 16, stride=16), :]

            def send(n, _):
                w = lax.rem(vert + n, VERT)
                pltpu.make_async_remote_copy(
                    rs2.at[w], r3.at[vert], mid_send.at[4], mid_recv.at[4], device_id=at(gz, w)
                ).start()
                return 0

            lax.fori_loop(1, VERT, send, 0)
            r3[vert] = rs2[vert]

        return 0

    lax.fori_loop(0, CHIPS, back_step, 0)

    @pl.when(core == MID)
    def _():
        pltpu.make_async_copy(r3.at[pl.ds(0, 7)], r3.at[pl.ds(0, 7)], mid_recv.at[4]).wait()
        total = None
        for bit in range(2):
            rows = r3[:, bit].reshape(L, L)

            out = jnp.dot(hot_t[bit], rows, precision=HIGH, preferred_element_type=F32)
            total = out if total is None else total + out
        xres[...] = total.reshape(32, 8, L)

        def send(n, _):
            w = lax.rem(gz + n, 32)
            pltpu.make_async_remote_copy(
                xres.at[w], res_in.at[p], mid_send.at[5], mid_recv.at[5], device_id=at(w, vert)
            ).start()
            return 0

        lax.fori_loop(1, 32, send, 0)
        pltpu.make_async_copy(xres.at[gz], res_in.at[p], loc_sem.at[3]).start()

    own_grad = pltpu.make_async_copy(gsend.at[p], grad_in.at[p], loc_sem.at[4])
    own_grad.start()

    pltpu.make_async_copy(abuf.at[pl.ds(0, 7)], abuf.at[pl.ds(0, 7)], ang_send).wait()
    pltpu.make_async_copy(xin.at[pl.ds(0, 15)], xin.at[pl.ds(0, 15)], vol_send).wait()

    @pl.when(core == MID)
    def _():
        pltpu.make_async_copy(mi.at[pl.ds(0, 15)], mi.at[pl.ds(0, 15)], mid_send.at[0]).wait()
        pltpu.make_async_copy(m2.at[pl.ds(0, 7)], m2.at[pl.ds(0, 7)], mid_send.at[1]).wait()
        pltpu.make_async_copy(m3.at[pl.ds(0, 15)], m3.at[pl.ds(0, 15)], mid_send.at[2]).wait()
        pltpu.make_async_copy(r3.at[pl.ds(0, 7)], r3.at[pl.ds(0, 7)], mid_send.at[4]).wait()
        pltpu.make_async_copy(xres.at[pl.ds(0, 31)], xres.at[pl.ds(0, 31)], mid_send.at[5]).wait()
        pltpu.make_async_copy(xres.at[gz], res_in.at[p], loc_sem.at[3]).wait()
        pltpu.make_async_copy(res_in.at[pl.ds(0, 15)], res_in.at[pl.ds(0, 15)], mid_recv.at[5]).wait()

    @pl.when(core != MID)
    def _():
        pltpu.make_async_copy(mi.at[pl.ds(0, 16)], mi.at[pl.ds(0, 16)], mid_send.at[0]).wait()
        pltpu.make_async_copy(res_in, res_in, mid_recv.at[5]).wait()

    @pl.when(own_mid)
    def _():
        pltpu.make_async_copy(rsend.at[pl.ds(0, 7)], rsend.at[pl.ds(0, 7)], mid_send.at[3]).wait()

    @pl.when(jnp.logical_not(own_mid))
    def _():
        pltpu.make_async_copy(rsend, rsend, mid_send.at[3]).wait()

    own_grad.wait()
    pltpu.make_async_copy(gsend.at[pl.ds(0, 15)], gsend.at[pl.ds(0, 15)], grad_send).wait()
    pltpu.make_async_copy(grad_in.at[pl.ds(0, 15)], grad_in.at[pl.ds(0, 15)], grad_recv).wait()


def exchange(volume, angles, det, measured):
    dma = pltpu.SemaphoreType.DMA
    hbm = pl.BlockSpec(memory_space=pltpu.HBM)
    vmem = lambda *dims, dtype=F32: pltpu.VMEM(dims, dtype)
    scratch = [
        vmem(8, 16, 1024), vmem(4, 4, 1024), vmem(16, 1024), vmem(1024, L), vmem(1024, L),
        vmem(CHIPS, 8, 8, L), vmem(CHIPS, 8, 8, L), vmem(VERT, 8, L, dtype=jnp.int32), vmem(VIEWS, L), vmem(VIEWS, L),
        vmem(4, VIEWS, L, dtype=jnp.int32), vmem(VIEWS, L, L), vmem(8 * EXT, L), vmem(VIEWS * 24, L),
        vmem(VIEWS, 8, L), vmem(VIEWS, 8, L), vmem(VIEWS, 8, L), vmem(L, L), vmem(32, 8, L), vmem(VERT, 2, 16, L),
        vmem(VERT, 2, 16, L), vmem(CHIPS, 16, L), vmem(CHIPS, 16, L), vmem(8, 16, L), vmem(CHIPS, 16, L),
        vmem(VERT, 2, 16, L), vmem(VERT, 2, 16, L), vmem(32, 8, L), vmem(CHIPS, 8, 8, L),
        vmem(VIEWS, 8, L), vmem(2, L, 2 * L), vmem(2, 2 * L, L), vmem(1, L, dtype=jnp.int32), pltpu.SMEM((4, VIEWS, L), jnp.int32), pltpu.SMEM((4,), jnp.int32),
        dma((5,)), dma, dma((CHIPS,)), dma, dma, dma, dma, dma((6,)), dma((6,)), dma, dma,
    ]
    return pl.pallas_call(
        kernel,
        out_shape=[jax.ShapeDtypeStruct((CHIPS, 8, 8, L), F32), jax.ShapeDtypeStruct((CHIPS, 8, L), F32)],
        in_specs=[hbm, hbm, hbm, hbm],
        out_specs=[hbm, hbm],
        scratch_shapes=scratch,
        compiler_params=pltpu.CompilerParams(collective_id=0, has_side_effects=True, vmem_limit_bytes=ALL_VMEM),
        name="exchange",
    )(volume, angles, det, measured)


def finish_kernel(grad_hbm, res_hbm, res_hbm_out, grad_hbm_out, grad_in, res_in, res_out, grad_out, turned, sem):
    load_r = pltpu.make_async_copy(res_hbm, res_in, sem.at[0])
    load_g = pltpu.make_async_copy(grad_hbm, grad_in, sem.at[1])
    load_r.start()
    load_g.start()
    load_r.wait()
    for r in range(8):
        both = jnp.concatenate([res_in[r], res_in[8 + r]], axis=0)
        turned[pl.ds(r, L, stride=8), 0:16] = jnp.transpose(both)
    for t in range(8):
        rows = jnp.transpose(turned[t * L : (t + 1) * L, 0:16])
        for a in range(4):
            res_out[a, :, t * L : (t + 1) * L] = rows[4 * a : 4 * a + 4]
    store_r = pltpu.make_async_copy(res_out, res_hbm_out, sem.at[2])
    store_r.start()
    load_g.wait()
    flat = grad_in.reshape(CHIPS * 64, L)
    for r in range(8):
        rows = [flat[pl.ds(zz * 8 + r, 16, stride=64), :] for zz in range(8)]
        turned[pl.ds(r, L, stride=8), :] = jnp.transpose(jnp.concatenate(rows, axis=0))
    for t in range(8):
        grad_out[:, :, t * L : (t + 1) * L] = jnp.transpose(turned[t * L : (t + 1) * L, :]).reshape(8, 16, L)
    store_g = pltpu.make_async_copy(grad_out, grad_hbm_out, sem.at[3])
    store_g.start()
    store_r.wait()
    store_g.wait()


def finish(grad_in, res_in):
    hbm = pl.BlockSpec(memory_space=pltpu.HBM)
    return pl.pallas_call(
        finish_kernel,
        out_shape=[jax.ShapeDtypeStruct((4, 4, 1024), F32), jax.ShapeDtypeStruct((8, 16, 1024), F32)],
        in_specs=[hbm, hbm],
        out_specs=[hbm, hbm],
        scratch_shapes=[
            pltpu.VMEM((CHIPS, 8, 8, L), F32), pltpu.VMEM((CHIPS, 8, L), F32), pltpu.VMEM((4, 4, 1024), F32),
            pltpu.VMEM((8, 16, 1024), F32), pltpu.VMEM((1024, L), F32), pltpu.SemaphoreType.DMA((4,)),
        ],
        compiler_params=pltpu.CompilerParams(vmem_limit_bytes=ALL_VMEM),
        name="finish",
    )(grad_in, res_in)


def per_device(volume, angle_index, detector_rows, measured):
    grad_in, res_in = exchange(volume, angle_index, detector_rows.reshape(1, L), measured)
    residual, gradient = finish(grad_in, res_in)
    return residual, gradient


def solution(mesh):
    in_specs = (P("gz", None, None), P("vert"), P(), P("vert", "gz", None))
    out_specs = (P("vert", "gz", None), P("gz", "vert", None))
    return jax.shard_map(per_device, mesh=mesh, in_specs=in_specs, out_specs=out_specs, check_vma=False)
```

```python
import jax
import jax.numpy as jnp
from jax import lax
from jax.experimental import pallas as pl
from jax.experimental.pallas import tpu as pltpu
from jax.sharding import PartitionSpec as P

L = 128
CHIPS = 16
VERT = 8
VIEWS = 32
GROUP = 8
AT_ONCE = 2
FORWARD_AT = 6
BACK_AT = 9
MID = 1
EXT = 56
F32 = jnp.float32
ALL_VMEM = 62 * 2**20
HIGH = lax.Precision.HIGHEST


def at(gz, vert):
    return {"gz": gz, "vert": vert}


def lane_iota(shape=(8, L)):
    return lax.broadcasted_iota(jnp.int32, shape, len(shape) - 1)


def sub_iota(shape=(8, L)):
    return lax.broadcasted_iota(jnp.int32, shape, len(shape) - 2)


def visit(i, p):
    step = lax.rem(i, 8)
    far = lax.div(step + 1, 2)
    dz = jnp.where(lax.rem(step, 2) == 1, far, 8 - far)
    z = lax.rem(lax.div(p, 2) + dz, 8)
    return z * 2 + lax.rem(p + lax.div(i, 8), 2)


def mixed(i):
    half = lax.div(i, 2)
    return jnp.where(i == CHIPS - 1, 0, jnp.where(lax.rem(i, 2) == 0, 1 + half, CHIPS - 1 - half))


def row_of(ref, r):
    return jnp.broadcast_to(ref[pl.ds(r, 1), :], (8, L))


def extend(x, ext, base):
    lane = lane_iota()
    zero = jnp.zeros((8, L), F32)
    r1, r2, r3 = (pltpu.roll(x, L - n, 1) for n in (1, 2, 3))
    parts = (
        x,
        jnp.where(lane < 127, r1, zero),
        jnp.where(lane < 126, r2, zero),
        jnp.where(lane < 126, x, zero),
        jnp.where(lane == 126, zero, r1),
        r2,
        jnp.where(lane == 125, zero, r3),
    )
    for n, value in enumerate(parts):
        ext[base + 8 * n : base + 8 * n + 8, :] = value


def project_slab(chunk, slab, ext, phi_t, tab, part, accs):
    lane = lane_iota()
    for zz in range(8):
        extend(chunk[zz], ext, zz * EXT)

    def some_views(g, _):
        offs = tab.at[0, pl.ds(g * GROUP, GROUP), pl.ds(slab * 8, 8)]
        phis = phi_t.at[pl.ds(g * GROUP, GROUP), pl.ds(slab * 8, 8), :]
        for j in range(GROUP):
            acc = None
            for zz in range(8):
                off = offs[j, zz]
                a = ext[pl.ds(off, 8), :]
                b = ext[pl.ds(off + 1, 8), :]
                term = a + row_of(phis.at[j], zz) * (b - a)
                acc = term if acc is None else acc + term
            accs[g * GROUP + j] = acc
        return 0

    lax.fori_loop(0, VIEWS // GROUP, some_views, 0)
    kcs = tab.at[1, :, pl.ds(slab * 8, 8)]
    for v in range(VIEWS):
        kc = kcs[v, 0]
        pos = lane + kc
        moved = pltpu.roll(accs[v], (L - kc) & (L - 1), 1)
        part[v] += jnp.where((pos >= -2) & (pos < L), moved, 0.0)


def backproject_slab(slab, bw, ext, phi_t, tab, out):
    lane = lane_iota()
    kcs = tab.at[3, :, pl.ds(slab * 8, 8)]
    for v in range(VIEWS):
        kc = kcs[v, 0]
        row = bw[v]
        for n in range(3):
            pos = lane + (kc + n)
            moved = pltpu.roll(row, (2 * L - kc - n) & (L - 1), 1)
            ext[v * 24 + 8 * n : v * 24 + 8 * n + 8, :] = jnp.where((pos >= 0) & (pos < L), moved, 0.0)

    def layers(n, _):
        offs = tab.at[2, :, pl.ds(slab * 8 + n * AT_ONCE, AT_ONCE)]
        phis = phi_t.at[:, pl.ds(slab * 8 + n * AT_ONCE, AT_ONCE), :]
        for zz in range(AT_ONCE):
            accs = [None] * 4
            for v in range(VIEWS):
                off = offs[v, zz]
                b = ext[pl.ds(off, 8), :]
                a = ext[pl.ds(off + 1, 8), :]
                term = a + row_of(phis.at[v], zz) * (b - a)
                accs[v % 4] = term if v < 4 else accs[v % 4] + term
            out[n * AT_ONCE + zz] = (accs[0] + accs[1]) + (accs[2] + accs[3])
        return 0

    lax.fori_loop(0, 8 // AT_ONCE, layers, 0)


def to_tiles(read, batch, turned, tiles):
    for t in range(8):
        turned[t * L : (t + 1) * L, 0:batch] = jnp.transpose(read(t))
    for r in range(8):
        tiles[r * batch : (r + 1) * batch, :] = jnp.transpose(turned[pl.ds(r, L, stride=8), 0:batch])


def one_hot(dr, bit):
    lane = lane_iota((8, L))
    wide = jnp.broadcast_to(dr, (8, L))
    halves = []
    for half in range(2):
        src = half * 64 + (lane // 8) * 4 + lane % 4
        got = jnp.take_along_axis(wide, src, axis=1, mode="promise_in_bounds")
        got = jnp.where((lane // 4) % 2 == bit, got, -1)
        halves.append(jnp.broadcast_to(got[0:1], (L, L)))
    row = lax.broadcasted_iota(jnp.int32, (L, 2 * L), 0)
    return (jnp.concatenate(halves, axis=1) == row).astype(F32)


def kernel(
    volume, angles_in, det_in, measured,
    grad_in, res_in,
    vb, mbuf, m16, turned, tiles, xsend, xin, abuf, sf, wt, tab_v, phi_t, ext, ext_b,
    part, pin, bw, mtiles, mi, mr, m2, msend, m3, rsend, r2, rs2, r3, xres, gsend, accs, hot, hot_t, det, tab, angles,
    loc_sem, vol_send, vol_recv, ang_send, ang_recv, part_send, part_recv,
    mid_send, mid_recv, grad_send, grad_recv,
):
    gz, vert = lax.axis_index("gz"), lax.axis_index("vert")
    p, core = lax.div(gz, 2), lax.rem(gz, 2)
    barrier = pltpu.get_barrier_semaphore()

    load_v = pltpu.make_async_copy(volume.at[:, pl.ds(pl.multiple_of(vert * 16, 16), 16), :], vb, loc_sem.at[0])
    load_m = pltpu.make_async_copy(measured, mbuf, loc_sem.at[1])
    load_a = pltpu.make_async_copy(angles_in, angles, loc_sem.at[3])
    load_d = pltpu.make_async_copy(det_in, det, loc_sem.at[4])
    for load in (load_a, load_v, load_m, load_d):
        load.start()

    def greet_gz(i, _):
        pl.semaphore_signal(barrier, inc=1, device_id=at(lax.rem(gz + i, 32), vert))
        return 0

    def greet_vert(i, _):
        pl.semaphore_signal(barrier, inc=1, device_id=at(gz, lax.rem(vert + i, VERT)))
        return 0

    lax.fori_loop(1, 32, greet_gz, 0)
    lax.fori_loop(1, VERT, greet_vert, 0)

    sub = sub_iota()
    load_a.wait()
    load_d.wait()
    slope = jnp.zeros((8, L), jnp.int32)
    for i in range(4):
        slope = jnp.where(sub % 4 == i, jnp.full((8, L), 2 * angles[i] - 512), slope)
    abuf[vert] = slope
    part[...] = jnp.zeros_like(part)

    load_m.wait()
    for a in range(4):
        m16[4 * a : 4 * a + 4, :] = mbuf[a]
    to_tiles(lambda t: m16[:, t * L : (t + 1) * L], 16, turned, mtiles)
    load_v.wait()
    to_tiles(lambda t: vb[:, :, t * L : (t + 1) * L].reshape(L, L), L, turned, tiles)

    def gather_rows(q, _):
        for zz in range(8):
            xsend[q, zz] = tiles[pl.ds(zz * 16 + q, 8, stride=L), :]
        return 0

    lax.fori_loop(0, CHIPS, gather_rows, 0)
    for zz in range(8):
        xin[p, zz] = xsend[p, zz]

    @pl.when(core == MID)
    def _():
        for bit in range(2):
            hot[bit] = one_hot(det[...], bit)
            hot_t[bit] = jnp.transpose(hot[bit])

    pl.semaphore_wait(barrier, 31 + 7)

    def send_angles(i, _):
        pltpu.make_async_remote_copy(
            abuf.at[vert], abuf.at[vert], ang_send, ang_recv, device_id=at(gz, lax.rem(vert + i, VERT))
        ).start()
        return 0

    lax.fori_loop(1, VERT, send_angles, 0)

    def measured_chunk(q):
        return mtiles.at[pl.ds(pl.multiple_of(lax.rem(q, 8) * 16 + lax.div(q, 8) * 8, 8), 8)]

    def send_measured(i, _):
        q = lax.rem(p + i, CHIPS)

        @pl.when(q * 2 + MID != gz)
        def _():
            pltpu.make_async_remote_copy(
                measured_chunk(q), mi.at[gz], mid_send.at[0], mid_recv.at[0], device_id=at(q * 2 + MID, vert)
            ).start()

        return 0

    lax.fori_loop(0, CHIPS, send_measured, 0)

    def vol_copy(i):
        q = visit(i, p)
        return pltpu.make_async_remote_copy(
            xsend.at[q], xin.at[p], vol_send, vol_recv.at[p], device_id=at(q * 2 + core, vert)
        )

    def send_volume(i, _):
        vol_copy(i).start()
        return 0

    lax.fori_loop(1, CHIPS, send_volume, 0)

    @pl.when(core == MID)
    def _():
        mi[gz] = measured_chunk(p)[...]

    pltpu.make_async_copy(abuf.at[pl.ds(0, 7)], abuf.at[pl.ds(0, 7)], ang_recv).wait()
    for g in range(4):
        tab_v[0, 8 * g : 8 * g + 8, :] = jnp.where(sub < 4, abuf[2 * g], abuf[2 * g + 1])
    s = tab_v[0]
    sf[...] = s.astype(F32)
    slope_value = sf[...] * (1.0 / 512)
    wt[...] = jnp.sqrt(1.0 + slope_value * slope_value)
    lane = lane_iota((VIEWS, L))
    first = 16 * (lane // 8) + 8 * core - 128
    ends = ((first * s) >> 9, ((first + 7) * s) >> 9)
    k_min, k_max = jnp.minimum(*ends), jnp.maximum(*ends)
    k = ((first + lane % 8) * s) >> 9
    kc = jnp.where(k_min < 0, jnp.minimum(k_min >> 3, -2), k_min >> 3)
    tab_v[0] = k - 8 * kc + jnp.where(k_min < 0, 24, 0) + (lane % 8) * EXT
    tab_v[1] = kc
    kb = (-k_max - 1) >> 3
    tab_v[2] = -k - 1 - 8 * kb + 24 * lax.broadcasted_iota(jnp.int32, (VIEWS, L), 0)
    tab_v[3] = kb
    to_smem = pltpu.make_async_copy(tab_v, tab, loc_sem.at[2])
    to_smem.start()

    def fill_phi(v, _):
        sv = row_of(sf, v)
        for slab in range(CHIPS):
            q = (16 * slab + 8 * core - 128 + sub).astype(F32) * sv * (1.0 / 512)
            phi_t[v, slab * 8 : slab * 8 + 8, :] = q - jnp.floor(q)
        return 0

    lax.fori_loop(0, VIEWS, fill_phi, 0)

    @pl.when(core == MID)
    def _():
        pltpu.make_async_copy(mi.at[pl.ds(0, 31)], mi.at[pl.ds(0, 31)], mid_recv.at[0]).wait()
        got = mi[...].reshape(2 * L, L)
        for bit in range(2):
            rows = jnp.dot(hot[bit], got, precision=HIGH, preferred_element_type=F32)
            mr[:, bit] = rows.reshape(VERT, 16, L)

        def send(n, _):
            w = lax.rem(vert + n, VERT)
            pltpu.make_async_remote_copy(
                mr.at[w], m2.at[vert], mid_send.at[1], mid_recv.at[1], device_id=at(gz, w)
            ).start()
            return 0

        lax.fori_loop(1, VERT, send, 0)
        m2[vert] = mr[vert]

    to_smem.wait()

    def project_step(i, _):
        q = visit(i, p)

        @pl.when(i > 0)
        def _():
            pltpu.make_async_copy(xin.at[q], xin.at[q], vol_recv.at[q]).wait()

        project_slab(xin.at[q], q, ext, phi_t, tab, part, accs)

        @pl.when((core == MID) & (i == FORWARD_AT))
        def _():
            pltpu.make_async_copy(m2.at[pl.ds(0, 7)], m2.at[pl.ds(0, 7)], mid_recv.at[1]).wait()
            flat = m2.reshape(256, L)
            for q in range(CHIPS):
                msend[q] = flat[pl.ds(q, 16, stride=16), :]

            def send(n, _):
                w = lax.rem(p + n, CHIPS)
                pltpu.make_async_remote_copy(
                    msend.at[w], m3.at[p], mid_send.at[2], mid_recv.at[2], device_id=at(w * 2 + MID, vert)
                ).start()
                return 0

            lax.fori_loop(1, CHIPS, send, 0)
            m3[p] = msend[p]

        return 0

    lax.fori_loop(0, CHIPS, project_step, 0)

    for v in range(VIEWS):
        part[v] = part[v] * row_of(wt, v)

    @pl.when(core == MID)
    def _():
        pltpu.make_async_copy(m3.at[pl.ds(0, 15)], m3.at[pl.ds(0, 15)], mid_recv.at[2]).wait()
        flat = m3.reshape(256, L)
        for v in range(VIEWS):
            w, pair, bit = v // 4, (v % 4) // 2, v % 2
            part[v] = part[v] - flat[pl.ds(pair * 128 + 2 * w + bit, 8, stride=16), :]

    swap = pltpu.make_async_remote_copy(part, pin, part_send, part_recv, device_id=at(gz + 1 - 2 * core, vert))
    swap.start()
    swap.wait()
    for v in range(VIEWS):
        value = (part[v] + pin[v]) * (1.0 / 16)
        pin[v] = value
        bw[v] = value * row_of(wt, v) * (VIEWS**-0.5)

    flat_res = pin.reshape(VIEWS * 8, L)
    for b in range(8):
        for bit in range(2):
            rsend[b, 8 * bit : 8 * bit + 8, :] = flat_res[pl.ds((2 * core + bit) * 8 + b, 8, stride=32), :]

    def send_residual(b, _):
        q = core * 8 + b

        @pl.when(q * 2 + MID != gz)
        def _():
            pltpu.make_async_remote_copy(
                rsend.at[b], r2.at[p], mid_send.at[3], mid_recv.at[3], device_id=at(q * 2 + MID, vert)
            ).start()

        return 0

    lax.fori_loop(0, 8, send_residual, 0)
    own_mid = (core == MID) & (lax.div(p, 8) == MID)

    @pl.when(own_mid)
    def _():
        r2[p] = rsend[lax.rem(p, 8)]

    def grad_copy(q):
        return pltpu.make_async_remote_copy(
            gsend.at[q], grad_in.at[p], grad_send, grad_recv, device_id=at(q * 2 + core, vert)
        )

    def back_step(i, _):
        q = visit(mixed(i), p)
        backproject_slab(q, bw, ext_b, phi_t, tab, gsend.at[q])

        @pl.when(i < CHIPS - 1)
        def _():
            grad_copy(q).start()

        @pl.when((core == MID) & (i == BACK_AT))
        def _():
            @pl.when(own_mid)
            def _():
                pltpu.make_async_copy(r2.at[pl.ds(0, 15)], r2.at[pl.ds(0, 15)], mid_recv.at[3]).wait()

            @pl.when(jnp.logical_not(own_mid))
            def _():
                pltpu.make_async_copy(r2, r2, mid_recv.at[3]).wait()

            flat = r2.reshape(256, L)
            for w in range(VERT):
                for bit in range(2):
                    rs2[w, bit] = flat[pl.ds(bit * 8 + w, 16, stride=16), :]

            def send(n, _):
                w = lax.rem(vert + n, VERT)
                pltpu.make_async_remote_copy(
                    rs2.at[w], r3.at[vert], mid_send.at[4], mid_recv.at[4], device_id=at(gz, w)
                ).start()
                return 0

            lax.fori_loop(1, VERT, send, 0)
            r3[vert] = rs2[vert]

        return 0

    lax.fori_loop(0, CHIPS, back_step, 0)

    @pl.when(core == MID)
    def _():
        pltpu.make_async_copy(r3.at[pl.ds(0, 7)], r3.at[pl.ds(0, 7)], mid_recv.at[4]).wait()
        total = None
        for bit in range(2):
            rows = r3[:, bit].reshape(L, L)

            out = jnp.dot(hot_t[bit], rows, precision=HIGH, preferred_element_type=F32)
            total = out if total is None else total + out
        xres[...] = total.reshape(32, 8, L)

        def send(n, _):
            w = lax.rem(gz + n, 32)
            pltpu.make_async_remote_copy(
                xres.at[w], res_in.at[p], mid_send.at[5], mid_recv.at[5], device_id=at(w, vert)
            ).start()
            return 0

        lax.fori_loop(1, 32, send, 0)
        pltpu.make_async_copy(xres.at[gz], res_in.at[p], loc_sem.at[3]).start()

    own_grad = pltpu.make_async_copy(gsend.at[p], grad_in.at[p], loc_sem.at[4])
    own_grad.start()

    pltpu.make_async_copy(abuf.at[pl.ds(0, 7)], abuf.at[pl.ds(0, 7)], ang_send).wait()
    pltpu.make_async_copy(xin.at[pl.ds(0, 15)], xin.at[pl.ds(0, 15)], vol_send).wait()

    @pl.when(core == MID)
    def _():
        pltpu.make_async_copy(mi.at[pl.ds(0, 15)], mi.at[pl.ds(0, 15)], mid_send.at[0]).wait()
        pltpu.make_async_copy(m2.at[pl.ds(0, 7)], m2.at[pl.ds(0, 7)], mid_send.at[1]).wait()
        pltpu.make_async_copy(m3.at[pl.ds(0, 15)], m3.at[pl.ds(0, 15)], mid_send.at[2]).wait()
        pltpu.make_async_copy(r3.at[pl.ds(0, 7)], r3.at[pl.ds(0, 7)], mid_send.at[4]).wait()
        pltpu.make_async_copy(xres.at[pl.ds(0, 31)], xres.at[pl.ds(0, 31)], mid_send.at[5]).wait()
        pltpu.make_async_copy(xres.at[gz], res_in.at[p], loc_sem.at[3]).wait()
        pltpu.make_async_copy(res_in.at[pl.ds(0, 15)], res_in.at[pl.ds(0, 15)], mid_recv.at[5]).wait()

    @pl.when(core != MID)
    def _():
        pltpu.make_async_copy(mi.at[pl.ds(0, 16)], mi.at[pl.ds(0, 16)], mid_send.at[0]).wait()
        pltpu.make_async_copy(res_in, res_in, mid_recv.at[5]).wait()

    @pl.when(own_mid)
    def _():
        pltpu.make_async_copy(rsend.at[pl.ds(0, 7)], rsend.at[pl.ds(0, 7)], mid_send.at[3]).wait()

    @pl.when(jnp.logical_not(own_mid))
    def _():
        pltpu.make_async_copy(rsend, rsend, mid_send.at[3]).wait()

    own_grad.wait()
    pltpu.make_async_copy(gsend.at[pl.ds(0, 15)], gsend.at[pl.ds(0, 15)], grad_send).wait()
    pltpu.make_async_copy(grad_in.at[pl.ds(0, 15)], grad_in.at[pl.ds(0, 15)], grad_recv).wait()


def exchange(volume, angles, det, measured):
    dma = pltpu.SemaphoreType.DMA
    hbm = pl.BlockSpec(memory_space=pltpu.HBM)
    vmem = lambda *dims, dtype=F32: pltpu.VMEM(dims, dtype)
    scratch = [
        vmem(8, 16, 1024), vmem(4, 4, 1024), vmem(16, 1024), vmem(1024, L), vmem(1024, L),
        vmem(CHIPS, 8, 8, L), vmem(CHIPS, 8, 8, L), vmem(VERT, 8, L, dtype=jnp.int32), vmem(VIEWS, L), vmem(VIEWS, L),
        vmem(4, VIEWS, L, dtype=jnp.int32), vmem(VIEWS, L, L), vmem(8 * EXT, L), vmem(VIEWS * 24, L),
        vmem(VIEWS, 8, L), vmem(VIEWS, 8, L), vmem(VIEWS, 8, L), vmem(L, L), vmem(32, 8, L), vmem(VERT, 2, 16, L),
        vmem(VERT, 2, 16, L), vmem(CHIPS, 16, L), vmem(CHIPS, 16, L), vmem(8, 16, L), vmem(CHIPS, 16, L),
        vmem(VERT, 2, 16, L), vmem(VERT, 2, 16, L), vmem(32, 8, L), vmem(CHIPS, 8, 8, L),
        vmem(VIEWS, 8, L), vmem(2, L, 2 * L), vmem(2, 2 * L, L), vmem(1, L, dtype=jnp.int32), pltpu.SMEM((4, VIEWS, L), jnp.int32), pltpu.SMEM((4,), jnp.int32),
        dma((5,)), dma, dma((CHIPS,)), dma, dma, dma, dma, dma((6,)), dma((6,)), dma, dma,
    ]
    return pl.pallas_call(
        kernel,
        out_shape=[jax.ShapeDtypeStruct((CHIPS, 8, 8, L), F32), jax.ShapeDtypeStruct((CHIPS, 8, L), F32)],
        in_specs=[hbm, hbm, hbm, hbm],
        out_specs=[hbm, hbm],
        scratch_shapes=scratch,
        compiler_params=pltpu.CompilerParams(collective_id=0, has_side_effects=True, vmem_limit_bytes=ALL_VMEM),
        name="exchange",
    )(volume, angles, det, measured)


def finish_kernel(grad_hbm, res_hbm, res_hbm_out, grad_hbm_out, grad_in, res_in, res_out, grad_out, turned, sem):
    load_r = pltpu.make_async_copy(res_hbm, res_in, sem.at[0])
    load_g = pltpu.make_async_copy(grad_hbm, grad_in, sem.at[1])
    load_r.start()
    load_g.start()
    load_r.wait()
    for r in range(8):
        both = jnp.concatenate([res_in[r], res_in[8 + r]], axis=0)
        turned[pl.ds(r, L, stride=8), 0:16] = jnp.transpose(both)
    for t in range(8):
        rows = jnp.transpose(turned[t * L : (t + 1) * L, 0:16])
        for a in range(4):
            res_out[a, :, t * L : (t + 1) * L] = rows[4 * a : 4 * a + 4]
    store_r = pltpu.make_async_copy(res_out, res_hbm_out, sem.at[2])
    store_r.start()
    load_g.wait()
    flat = grad_in.reshape(CHIPS * 64, L)
    for r in range(8):
        rows = [flat[pl.ds(zz * 8 + r, 16, stride=64), :] for zz in range(8)]
        turned[pl.ds(r, L, stride=8), :] = jnp.transpose(jnp.concatenate(rows, axis=0))
    for t in range(8):
        grad_out[:, :, t * L : (t + 1) * L] = jnp.transpose(turned[t * L : (t + 1) * L, :]).reshape(8, 16, L)
    store_g = pltpu.make_async_copy(grad_out, grad_hbm_out, sem.at[3])
    store_g.start()
    store_r.wait()
    store_g.wait()


def finish(grad_in, res_in):
    hbm = pl.BlockSpec(memory_space=pltpu.HBM)
    return pl.pallas_call(
        finish_kernel,
        out_shape=[jax.ShapeDtypeStruct((4, 4, 1024), F32), jax.ShapeDtypeStruct((8, 16, 1024), F32)],
        in_specs=[hbm, hbm],
        out_specs=[hbm, hbm],
        scratch_shapes=[
            pltpu.VMEM((CHIPS, 8, 8, L), F32), pltpu.VMEM((CHIPS, 8, L), F32), pltpu.VMEM((4, 4, 1024), F32),
            pltpu.VMEM((8, 16, 1024), F32), pltpu.VMEM((1024, L), F32), pltpu.SemaphoreType.DMA((4,)),
        ],
        compiler_params=pltpu.CompilerParams(vmem_limit_bytes=ALL_VMEM),
        name="finish",
    )(grad_in, res_in)


def per_device(volume, angle_index, detector_rows, measured):
    grad_in, res_in = exchange(volume, angle_index, detector_rows.reshape(1, L), measured)
    residual, gradient = finish(grad_in, res_in)
    return residual, gradient


def solution(mesh):
    in_specs = (P("gz", None, None), P("vert"), P(), P("vert", "gz", None))
    out_specs = (P("vert", "gz", None), P("gz", "vert", None))
    return jax.shard_map(per_device, mesh=mesh, in_specs=in_specs, out_specs=out_specs, check_vma=False)
```

```python
import jax
import jax.numpy as jnp
from jax import lax
from jax.experimental import pallas as pl
from jax.experimental.pallas import tpu as pltpu
from jax.sharding import PartitionSpec as P

L = 128
CHIPS = 16
VERT = 8
VIEWS = 32
GROUP = 16
AT_ONCE = 4
FORWARD_AT = 8
BACK_AT = 9
MID = 1
EXT = 56
F32 = jnp.float32
ALL_VMEM = 62 * 2**20
HIGH = lax.Precision.HIGHEST


def at(gz, vert):
    return {"gz": gz, "vert": vert}


def lane_iota(shape=(8, L)):
    return lax.broadcasted_iota(jnp.int32, shape, len(shape) - 1)


def sub_iota(shape=(8, L)):
    return lax.broadcasted_iota(jnp.int32, shape, len(shape) - 2)


def visit(i, p):
    step = lax.rem(i, 8)
    far = lax.div(step + 1, 2)
    dz = jnp.where(lax.rem(step, 2) == 1, far, 8 - far)
    z = lax.rem(lax.div(p, 2) + dz, 8)
    return z * 2 + lax.rem(p + lax.div(i, 8), 2)


def mixed(i):
    half = lax.div(i, 2)
    return jnp.where(i == CHIPS - 1, 0, jnp.where(lax.rem(i, 2) == 0, 1 + half, CHIPS - 1 - half))


def row_of(ref, r):
    return jnp.broadcast_to(ref[pl.ds(r, 1), :], (8, L))


def extend(x, ext, base):
    lane = lane_iota()
    zero = jnp.zeros((8, L), F32)
    r1, r2, r3 = (pltpu.roll(x, L - n, 1) for n in (1, 2, 3))
    parts = (
        x,
        jnp.where(lane < 127, r1, zero),
        jnp.where(lane < 126, r2, zero),
        jnp.where(lane < 126, x, zero),
        jnp.where(lane == 126, zero, r1),
        r2,
        jnp.where(lane == 125, zero, r3),
    )
    for n, value in enumerate(parts):
        ext[base + 8 * n : base + 8 * n + 8, :] = value


def project_slab(chunk, slab, ext, phi_t, tab, part, accs):
    lane = lane_iota()
    for zz in range(8):
        extend(chunk[zz], ext, zz * EXT)

    def some_views(g, _):
        offs = tab.at[0, pl.ds(g * GROUP, GROUP), pl.ds(slab * 8, 8)]
        phis = phi_t.at[pl.ds(g * GROUP, GROUP), pl.ds(slab * 8, 8), :]
        for j in range(GROUP):
            acc = None
            for zz in range(8):
                off = offs[j, zz]
                a = ext[pl.ds(off, 8), :]
                b = ext[pl.ds(off + 1, 8), :]
                term = a + row_of(phis.at[j], zz) * (b - a)
                acc = term if acc is None else acc + term
            accs[g * GROUP + j] = acc
        return 0

    lax.fori_loop(0, VIEWS // GROUP, some_views, 0)
    kcs = tab.at[1, :, pl.ds(slab * 8, 8)]
    for v in range(VIEWS):
        kc = kcs[v, 0]
        pos = lane + kc
        moved = pltpu.roll(accs[v], (L - kc) & (L - 1), 1)
        part[v] += jnp.where((pos >= -2) & (pos < L), moved, 0.0)


def backproject_slab(slab, bw, ext, phi_t, tab, out):
    lane = lane_iota()
    kcs = tab.at[3, :, pl.ds(slab * 8, 8)]
    for v in range(VIEWS):
        kc = kcs[v, 0]
        row = bw[v]
        for n in range(3):
            pos = lane + (kc + n)
            moved = pltpu.roll(row, (2 * L - kc - n) & (L - 1), 1)
            ext[v * 24 + 8 * n : v * 24 + 8 * n + 8, :] = jnp.where((pos >= 0) & (pos < L), moved, 0.0)

    def layers(n, _):
        offs = tab.at[2, :, pl.ds(slab * 8 + n * AT_ONCE, AT_ONCE)]
        phis = phi_t.at[:, pl.ds(slab * 8 + n * AT_ONCE, AT_ONCE), :]
        for zz in range(AT_ONCE):
            accs = [None] * 4
            for v in range(VIEWS):
                off = offs[v, zz]
                b = ext[pl.ds(off, 8), :]
                a = ext[pl.ds(off + 1, 8), :]
                term = a + row_of(phis.at[v], zz) * (b - a)
                accs[v % 4] = term if v < 4 else accs[v % 4] + term
            out[n * AT_ONCE + zz] = (accs[0] + accs[1]) + (accs[2] + accs[3])
        return 0

    lax.fori_loop(0, 8 // AT_ONCE, layers, 0)


def to_tiles(read, batch, turned, tiles):
    for t in range(8):
        turned[t * L : (t + 1) * L, 0:batch] = jnp.transpose(read(t))
    for r in range(8):
        tiles[r * batch : (r + 1) * batch, :] = jnp.transpose(turned[pl.ds(r, L, stride=8), 0:batch])


def one_hot(dr, bit):
    lane = lane_iota((8, L))
    wide = jnp.broadcast_to(dr, (8, L))
    halves = []
    for half in range(2):
        src = half * 64 + (lane // 8) * 4 + lane % 4
        got = jnp.take_along_axis(wide, src, axis=1, mode="promise_in_bounds")
        got = jnp.where((lane // 4) % 2 == bit, got, -1)
        halves.append(jnp.broadcast_to(got[0:1], (L, L)))
    row = lax.broadcasted_iota(jnp.int32, (L, 2 * L), 0)
    return (jnp.concatenate(halves, axis=1) == row).astype(F32)


def kernel(
    volume, angles_in, det_in, measured,
    grad_in, res_in,
    vb, mbuf, m16, turned, tiles, xsend, xin, abuf, sf, wt, tab_v, phi_t, ext, ext_b,
    part, pin, bw, mtiles, mi, mr, m2, msend, m3, rsend, r2, rs2, r3, xres, gsend, accs, hot, hot_t, det, tab, angles,
    loc_sem, vol_send, vol_recv, ang_send, ang_recv, part_send, part_recv,
    mid_send, mid_recv, grad_send, grad_recv,
):
    gz, vert = lax.axis_index("gz"), lax.axis_index("vert")
    p, core = lax.div(gz, 2), lax.rem(gz, 2)
    barrier = pltpu.get_barrier_semaphore()

    load_v = pltpu.make_async_copy(volume.at[:, pl.ds(pl.multiple_of(vert * 16, 16), 16), :], vb, loc_sem.at[0])
    load_m = pltpu.make_async_copy(measured, mbuf, loc_sem.at[1])
    load_a = pltpu.make_async_copy(angles_in, angles, loc_sem.at[3])
    load_d = pltpu.make_async_copy(det_in, det, loc_sem.at[4])
    for load in (load_a, load_v, load_m, load_d):
        load.start()

    def greet_gz(i, _):
        pl.semaphore_signal(barrier, inc=1, device_id=at(lax.rem(gz + i, 32), vert))
        return 0

    def greet_vert(i, _):
        pl.semaphore_signal(barrier, inc=1, device_id=at(gz, lax.rem(vert + i, VERT)))
        return 0

    lax.fori_loop(1, 32, greet_gz, 0)
    lax.fori_loop(1, VERT, greet_vert, 0)

    sub = sub_iota()
    load_a.wait()
    load_d.wait()
    slope = jnp.zeros((8, L), jnp.int32)
    for i in range(4):
        slope = jnp.where(sub % 4 == i, jnp.full((8, L), 2 * angles[i] - 512), slope)
    abuf[vert] = slope
    part[...] = jnp.zeros_like(part)

    load_m.wait()
    for a in range(4):
        m16[4 * a : 4 * a + 4, :] = mbuf[a]
    to_tiles(lambda t: m16[:, t * L : (t + 1) * L], 16, turned, mtiles)
    load_v.wait()
    to_tiles(lambda t: vb[:, :, t * L : (t + 1) * L].reshape(L, L), L, turned, tiles)

    def gather_rows(q, _):
        for zz in range(8):
            xsend[q, zz] = tiles[pl.ds(zz * 16 + q, 8, stride=L), :]
        return 0

    lax.fori_loop(0, CHIPS, gather_rows, 0)
    for zz in range(8):
        xin[p, zz] = xsend[p, zz]

    @pl.when(core == MID)
    def _():
        for bit in range(2):
            hot[bit] = one_hot(det[...], bit)
            hot_t[bit] = jnp.transpose(hot[bit])

    pl.semaphore_wait(barrier, 31 + 7)

    def send_angles(i, _):
        pltpu.make_async_remote_copy(
            abuf.at[vert], abuf.at[vert], ang_send, ang_recv, device_id=at(gz, lax.rem(vert + i, VERT))
        ).start()
        return 0

    lax.fori_loop(1, VERT, send_angles, 0)

    def measured_chunk(q):
        return mtiles.at[pl.ds(pl.multiple_of(lax.rem(q, 8) * 16 + lax.div(q, 8) * 8, 8), 8)]

    def send_measured(i, _):
        q = lax.rem(p + i, CHIPS)

        @pl.when(q * 2 + MID != gz)
        def _():
            pltpu.make_async_remote_copy(
                measured_chunk(q), mi.at[gz], mid_send.at[0], mid_recv.at[0], device_id=at(q * 2 + MID, vert)
            ).start()

        return 0

    lax.fori_loop(0, CHIPS, send_measured, 0)

    def vol_copy(i):
        q = visit(i, p)
        return pltpu.make_async_remote_copy(
            xsend.at[q], xin.at[p], vol_send, vol_recv.at[p], device_id=at(q * 2 + core, vert)
        )

    def send_volume(i, _):
        vol_copy(i).start()
        return 0

    lax.fori_loop(1, CHIPS, send_volume, 0)

    @pl.when(core == MID)
    def _():
        mi[gz] = measured_chunk(p)[...]

    pltpu.make_async_copy(abuf.at[pl.ds(0, 7)], abuf.at[pl.ds(0, 7)], ang_recv).wait()
    for g in range(4):
        tab_v[0, 8 * g : 8 * g + 8, :] = jnp.where(sub < 4, abuf[2 * g], abuf[2 * g + 1])
    s = tab_v[0]
    sf[...] = s.astype(F32)
    slope_value = sf[...] * (1.0 / 512)
    wt[...] = jnp.sqrt(1.0 + slope_value * slope_value)
    lane = lane_iota((VIEWS, L))
    first = 16 * (lane // 8) + 8 * core - 128
    ends = ((first * s) >> 9, ((first + 7) * s) >> 9)
    k_min, k_max = jnp.minimum(*ends), jnp.maximum(*ends)
    k = ((first + lane % 8) * s) >> 9
    kc = jnp.where(k_min < 0, jnp.minimum(k_min >> 3, -2), k_min >> 3)
    tab_v[0] = k - 8 * kc + jnp.where(k_min < 0, 24, 0) + (lane % 8) * EXT
    tab_v[1] = kc
    kb = (-k_max - 1) >> 3
    tab_v[2] = -k - 1 - 8 * kb + 24 * lax.broadcasted_iota(jnp.int32, (VIEWS, L), 0)
    tab_v[3] = kb
    to_smem = pltpu.make_async_copy(tab_v, tab, loc_sem.at[2])
    to_smem.start()

    def fill_phi(v, _):
        sv = row_of(sf, v)
        for slab in range(CHIPS):
            q = (16 * slab + 8 * core - 128 + sub).astype(F32) * sv * (1.0 / 512)
            phi_t[v, slab * 8 : slab * 8 + 8, :] = q - jnp.floor(q)
        return 0

    lax.fori_loop(0, VIEWS, fill_phi, 0)

    @pl.when(core == MID)
    def _():
        pltpu.make_async_copy(mi.at[pl.ds(0, 31)], mi.at[pl.ds(0, 31)], mid_recv.at[0]).wait()
        got = mi[...].reshape(2 * L, L)
        for bit in range(2):
            rows = jnp.dot(hot[bit], got, precision=HIGH, preferred_element_type=F32)
            mr[:, bit] = rows.reshape(VERT, 16, L)

        def send(n, _):
            w = lax.rem(vert + n, VERT)
            pltpu.make_async_remote_copy(
                mr.at[w], m2.at[vert], mid_send.at[1], mid_recv.at[1], device_id=at(gz, w)
            ).start()
            return 0

        lax.fori_loop(1, VERT, send, 0)
        m2[vert] = mr[vert]

    to_smem.wait()

    def project_step(i, _):
        q = visit(i, p)

        @pl.when(i > 0)
        def _():
            pltpu.make_async_copy(xin.at[q], xin.at[q], vol_recv.at[q]).wait()

        project_slab(xin.at[q], q, ext, phi_t, tab, part, accs)

        @pl.when((core == MID) & (i == FORWARD_AT))
        def _():
            pltpu.make_async_copy(m2.at[pl.ds(0, 7)], m2.at[pl.ds(0, 7)], mid_recv.at[1]).wait()
            flat = m2.reshape(256, L)
            for q in range(CHIPS):
                msend[q] = flat[pl.ds(q, 16, stride=16), :]

            def send(n, _):
                w = lax.rem(p + n, CHIPS)
                pltpu.make_async_remote_copy(
                    msend.at[w], m3.at[p], mid_send.at[2], mid_recv.at[2], device_id=at(w * 2 + MID, vert)
                ).start()
                return 0

            lax.fori_loop(1, CHIPS, send, 0)
            m3[p] = msend[p]

        return 0

    lax.fori_loop(0, CHIPS, project_step, 0)

    for v in range(VIEWS):
        part[v] = part[v] * row_of(wt, v)

    @pl.when(core == MID)
    def _():
        pltpu.make_async_copy(m3.at[pl.ds(0, 15)], m3.at[pl.ds(0, 15)], mid_recv.at[2]).wait()
        flat = m3.reshape(256, L)
        for v in range(VIEWS):
            w, pair, bit = v // 4, (v % 4) // 2, v % 2
            part[v] = part[v] - flat[pl.ds(pair * 128 + 2 * w + bit, 8, stride=16), :]

    swap = pltpu.make_async_remote_copy(part, pin, part_send, part_recv, device_id=at(gz + 1 - 2 * core, vert))
    swap.start()
    swap.wait()
    for v in range(VIEWS):
        value = (part[v] + pin[v]) * (1.0 / 16)
        pin[v] = value
        bw[v] = value * row_of(wt, v) * (VIEWS**-0.5)

    flat_res = pin.reshape(VIEWS * 8, L)
    for b in range(8):
        for bit in range(2):
            rsend[b, 8 * bit : 8 * bit + 8, :] = flat_res[pl.ds((2 * core + bit) * 8 + b, 8, stride=32), :]

    def send_residual(b, _):
        q = core * 8 + b

        @pl.when(q * 2 + MID != gz)
        def _():
            pltpu.make_async_remote_copy(
                rsend.at[b], r2.at[p], mid_send.at[3], mid_recv.at[3], device_id=at(q * 2 + MID, vert)
            ).start()

        return 0

    lax.fori_loop(0, 8, send_residual, 0)
    own_mid = (core == MID) & (lax.div(p, 8) == MID)

    @pl.when(own_mid)
    def _():
        r2[p] = rsend[lax.rem(p, 8)]

    def grad_copy(q):
        return pltpu.make_async_remote_copy(
            gsend.at[q], grad_in.at[p], grad_send, grad_recv, device_id=at(q * 2 + core, vert)
        )

    def back_step(i, _):
        q = visit(mixed(i), p)
        backproject_slab(q, bw, ext_b, phi_t, tab, gsend.at[q])

        @pl.when(i < CHIPS - 1)
        def _():
            grad_copy(q).start()

        @pl.when((core == MID) & (i == BACK_AT))
        def _():
            @pl.when(own_mid)
            def _():
                pltpu.make_async_copy(r2.at[pl.ds(0, 15)], r2.at[pl.ds(0, 15)], mid_recv.at[3]).wait()

            @pl.when(jnp.logical_not(own_mid))
            def _():
                pltpu.make_async_copy(r2, r2, mid_recv.at[3]).wait()

            flat = r2.reshape(256, L)
            for w in range(VERT):
                for bit in range(2):
                    rs2[w, bit] = flat[pl.ds(bit * 8 + w, 16, stride=16), :]

            def send(n, _):
                w = lax.rem(vert + n, VERT)
                pltpu.make_async_remote_copy(
                    rs2.at[w], r3.at[vert], mid_send.at[4], mid_recv.at[4], device_id=at(gz, w)
                ).start()
                return 0

            lax.fori_loop(1, VERT, send, 0)
            r3[vert] = rs2[vert]

        return 0

    lax.fori_loop(0, CHIPS, back_step, 0)

    @pl.when(core == MID)
    def _():
        pltpu.make_async_copy(r3.at[pl.ds(0, 7)], r3.at[pl.ds(0, 7)], mid_recv.at[4]).wait()
        total = None
        for bit in range(2):
            rows = r3[:, bit].reshape(L, L)

            out = jnp.dot(hot_t[bit], rows, precision=HIGH, preferred_element_type=F32)
            total = out if total is None else total + out
        xres[...] = total.reshape(32, 8, L)

        def send(n, _):
            w = lax.rem(gz + n, 32)
            pltpu.make_async_remote_copy(
                xres.at[w], res_in.at[p], mid_send.at[5], mid_recv.at[5], device_id=at(w, vert)
            ).start()
            return 0

        lax.fori_loop(1, 32, send, 0)
        pltpu.make_async_copy(xres.at[gz], res_in.at[p], loc_sem.at[3]).start()

    own_grad = pltpu.make_async_copy(gsend.at[p], grad_in.at[p], loc_sem.at[4])
    own_grad.start()

    pltpu.make_async_copy(abuf.at[pl.ds(0, 7)], abuf.at[pl.ds(0, 7)], ang_send).wait()
    pltpu.make_async_copy(xin.at[pl.ds(0, 15)], xin.at[pl.ds(0, 15)], vol_send).wait()

    @pl.when(core == MID)
    def _():
        pltpu.make_async_copy(mi.at[pl.ds(0, 15)], mi.at[pl.ds(0, 15)], mid_send.at[0]).wait()
        pltpu.make_async_copy(m2.at[pl.ds(0, 7)], m2.at[pl.ds(0, 7)], mid_send.at[1]).wait()
        pltpu.make_async_copy(m3.at[pl.ds(0, 15)], m3.at[pl.ds(0, 15)], mid_send.at[2]).wait()
        pltpu.make_async_copy(r3.at[pl.ds(0, 7)], r3.at[pl.ds(0, 7)], mid_send.at[4]).wait()
        pltpu.make_async_copy(xres.at[pl.ds(0, 31)], xres.at[pl.ds(0, 31)], mid_send.at[5]).wait()
        pltpu.make_async_copy(xres.at[gz], res_in.at[p], loc_sem.at[3]).wait()
        pltpu.make_async_copy(res_in.at[pl.ds(0, 15)], res_in.at[pl.ds(0, 15)], mid_recv.at[5]).wait()

    @pl.when(core != MID)
    def _():
        pltpu.make_async_copy(mi.at[pl.ds(0, 16)], mi.at[pl.ds(0, 16)], mid_send.at[0]).wait()
        pltpu.make_async_copy(res_in, res_in, mid_recv.at[5]).wait()

    @pl.when(own_mid)
    def _():
        pltpu.make_async_copy(rsend.at[pl.ds(0, 7)], rsend.at[pl.ds(0, 7)], mid_send.at[3]).wait()

    @pl.when(jnp.logical_not(own_mid))
    def _():
        pltpu.make_async_copy(rsend, rsend, mid_send.at[3]).wait()

    own_grad.wait()
    pltpu.make_async_copy(gsend.at[pl.ds(0, 15)], gsend.at[pl.ds(0, 15)], grad_send).wait()
    pltpu.make_async_copy(grad_in.at[pl.ds(0, 15)], grad_in.at[pl.ds(0, 15)], grad_recv).wait()


def exchange(volume, angles, det, measured):
    dma = pltpu.SemaphoreType.DMA
    hbm = pl.BlockSpec(memory_space=pltpu.HBM)
    vmem = lambda *dims, dtype=F32: pltpu.VMEM(dims, dtype)
    scratch = [
        vmem(8, 16, 1024), vmem(4, 4, 1024), vmem(16, 1024), vmem(1024, L), vmem(1024, L),
        vmem(CHIPS, 8, 8, L), vmem(CHIPS, 8, 8, L), vmem(VERT, 8, L, dtype=jnp.int32), vmem(VIEWS, L), vmem(VIEWS, L),
        vmem(4, VIEWS, L, dtype=jnp.int32), vmem(VIEWS, L, L), vmem(8 * EXT, L), vmem(VIEWS * 24, L),
        vmem(VIEWS, 8, L), vmem(VIEWS, 8, L), vmem(VIEWS, 8, L), vmem(L, L), vmem(32, 8, L), vmem(VERT, 2, 16, L),
        vmem(VERT, 2, 16, L), vmem(CHIPS, 16, L), vmem(CHIPS, 16, L), vmem(8, 16, L), vmem(CHIPS, 16, L),
        vmem(VERT, 2, 16, L), vmem(VERT, 2, 16, L), vmem(32, 8, L), vmem(CHIPS, 8, 8, L),
        vmem(VIEWS, 8, L), vmem(2, L, 2 * L), vmem(2, 2 * L, L), vmem(1, L, dtype=jnp.int32), pltpu.SMEM((4, VIEWS, L), jnp.int32), pltpu.SMEM((4,), jnp.int32),
        dma((5,)), dma, dma((CHIPS,)), dma, dma, dma, dma, dma((6,)), dma((6,)), dma, dma,
    ]
    return pl.pallas_call(
        kernel,
        out_shape=[jax.ShapeDtypeStruct((CHIPS, 8, 8, L), F32), jax.ShapeDtypeStruct((CHIPS, 8, L), F32)],
        in_specs=[hbm, hbm, hbm, hbm],
        out_specs=[hbm, hbm],
        scratch_shapes=scratch,
        compiler_params=pltpu.CompilerParams(collective_id=0, has_side_effects=True, vmem_limit_bytes=ALL_VMEM),
        name="exchange",
    )(volume, angles, det, measured)


def finish_kernel(grad_hbm, res_hbm, res_hbm_out, grad_hbm_out, grad_in, res_in, res_out, grad_out, turned, sem):
    load_r = pltpu.make_async_copy(res_hbm, res_in, sem.at[0])
    load_g = pltpu.make_async_copy(grad_hbm, grad_in, sem.at[1])
    load_r.start()
    load_g.start()
    load_r.wait()
    for r in range(8):
        both = jnp.concatenate([res_in[r], res_in[8 + r]], axis=0)
        turned[pl.ds(r, L, stride=8), 0:16] = jnp.transpose(both)
    for t in range(8):
        rows = jnp.transpose(turned[t * L : (t + 1) * L, 0:16])
        for a in range(4):
            res_out[a, :, t * L : (t + 1) * L] = rows[4 * a : 4 * a + 4]
    store_r = pltpu.make_async_copy(res_out, res_hbm_out, sem.at[2])
    store_r.start()
    load_g.wait()
    flat = grad_in.reshape(CHIPS * 64, L)
    for r in range(8):
        rows = [flat[pl.ds(zz * 8 + r, 16, stride=64), :] for zz in range(8)]
        turned[pl.ds(r, L, stride=8), :] = jnp.transpose(jnp.concatenate(rows, axis=0))
    for t in range(8):
        grad_out[:, :, t * L : (t + 1) * L] = jnp.transpose(turned[t * L : (t + 1) * L, :]).reshape(8, 16, L)
    store_g = pltpu.make_async_copy(grad_out, grad_hbm_out, sem.at[3])
    store_g.start()
    store_r.wait()
    store_g.wait()


def finish(grad_in, res_in):
    hbm = pl.BlockSpec(memory_space=pltpu.HBM)
    return pl.pallas_call(
        finish_kernel,
        out_shape=[jax.ShapeDtypeStruct((4, 4, 1024), F32), jax.ShapeDtypeStruct((8, 16, 1024), F32)],
        in_specs=[hbm, hbm],
        out_specs=[hbm, hbm],
        scratch_shapes=[
            pltpu.VMEM((CHIPS, 8, 8, L), F32), pltpu.VMEM((CHIPS, 8, L), F32), pltpu.VMEM((4, 4, 1024), F32),
            pltpu.VMEM((8, 16, 1024), F32), pltpu.VMEM((1024, L), F32), pltpu.SemaphoreType.DMA((4,)),
        ],
        compiler_params=pltpu.CompilerParams(vmem_limit_bytes=ALL_VMEM),
        name="finish",
    )(grad_in, res_in)


def per_device(volume, angle_index, detector_rows, measured):
    grad_in, res_in = exchange(volume, angle_index, detector_rows.reshape(1, L), measured)
    residual, gradient = finish(grad_in, res_in)
    return residual, gradient


def solution(mesh):
    in_specs = (P("gz", None, None), P("vert"), P(), P("vert", "gz", None))
    out_specs = (P("vert", "gz", None), P("gz", "vert", None))
    return jax.shard_map(per_device, mesh=mesh, in_specs=in_specs, out_specs=out_specs, check_vma=False)
```
